32 devices in a mesh: gx: 8 (over z, y), gy: 4 (over x, core).
Axes of the slice: x: 2, y: 2, z: 4, core: 2. Of those that a mesh axis runs over, the one named last changes fastest.
Arguments:
- populations: float32 [27, 16, 32, 128], P(None, 'gx', 'gy'), as said below
- relax: float32 [27], replicated, may hold values from 0.6 to 1.9
- solid: int32 [16, 32, 128], P('gx', 'gy'), may hold values 0 or 1
- wall_cell: int32 [8, 4, 256], P('gx', 'gy'), may hold values from 0 to 2047, as said below
- wall_normal: int32 [8, 4, 256], P('gx', 'gy'), may hold values from 0 to 5
- wall_count: int32 [8, 4], P('gx', 'gy'), may hold values from 1 to 256, as said below
- sample_ref: int32 [8, 4, 256], P('gx', 'gy'), may hold values from 0 to 255, each once within a row
- stencil_cell: int32 [8, 4, 8, 256], P('gx', 'gy'), may hold values from 0 to 2047, as said below
- stencil_weight: float32 [8, 4, 8, 256], P('gx', 'gy'), may hold values from 0 to 1, as said below
Outputs:
- read: float32 [27, 16, 32, 128], P(None, 'gx', 'gy')
The draws below stay inside these ranges and needn't reach their ends.
Inputs may be any that keep to these rules, and one draw needn't show every extreme that they name: `populations`: positive everywhere. `wall_cell`: the 256 entries of one device are distinct local cells. Slots 0 to wall_count - 1 of a device are live; some device has all 256 live. `stencil_cell`: the eight corners of a unit cube of the owner's local cells, wrapping along z only. `stencil_weight`: nonnegative trilinear weights, summing to one over the eight corners.
All inputs are finite; a program needn't handle non-finite values. No bound on the sum of `solid` on one device may be relied on, other than what follows from the above.
Results may differ from the reference program's by a relative error of at most 0.0003.
Values sent between devices are 32-bit elements; how exact they have to be, the bound alone decides.
A program may use at most 64 MiB of HBM per device.

```python
import math
import jax
import jax.numpy as jnp
import numpy as np
from jax import lax

CX = 2
CY = 8
NZ = 128
SLOTS = 64
WALL = 256
NX = 16
NY = 32
N_GX = 8
N_GY = 4


def draw_populations(key, part):
    base = jax.random.fold_in(key, 101)
    steps = np.array([(a - 1, b - 1, c - 1) for a in range(3) for b in range(3) for c in range(3)]).T
    drift = np.array([0.06, 0.02, -0.02])
    projected = drift @ steps
    resting = 1.0 + 3.0 * projected + 4.5 * projected * projected - 1.5 * np.sum(drift * drift)
    shape = (27, NX, NY, NZ)
    noise = 0.12 * jnp.clip(jax.random.normal(base, shape, jnp.float32), -3.5, 3.5)
    return (jnp.asarray(resting, jnp.float32).reshape(27, 1, 1, 1) * (1.0 + noise)).astype(jnp.float32)


def draw_stencil_cell(key, part):
    grid_x = NX // CX
    grid_y = NY // CY
    shape = (grid_x, grid_y, 1, WALL)
    first, second, third = jax.random.split(jax.random.fold_in(key, 202), 3)
    base_x = jax.random.randint(first, shape, 0, CX - 1)
    base_y = jax.random.randint(second, shape, 0, CY - 1)
    base_z = jax.random.randint(third, shape, 0, NZ)
    corner = jnp.arange(8, dtype=jnp.int32).reshape(1, 1, 8, 1)
    offset_x = corner // 4
    offset_y = corner // 2 % 2
    offset_z = corner % 2
    cells = ((base_x + offset_x) * CY + base_y + offset_y) * NZ + (base_z + offset_z) % NZ
    return cells.astype(jnp.int32)


def draw_stencil_weight(key, part):
    grid_x = NX // CX
    grid_y = NY // CY
    shape = (grid_x, grid_y, 3, 1, WALL)
    base = jax.random.fold_in(key, 303)
    fraction = jax.random.uniform(base, shape, jnp.float32, 0.0, 1.0)
    corner = jnp.arange(8, dtype=jnp.int32)
    bits = jnp.stack([corner // 4, corner // 2 % 2, corner % 2]).reshape(1, 1, 3, 8, 1)
    factor = jnp.where(bits == 1, fraction, 1.0 - fraction)
    return jnp.prod(factor, axis=2).astype(jnp.float32)


def draw_wall_cell(key, part):
    grid_x = NX // CX
    grid_y = NY // CY
    keys = jax.random.split(jax.random.fold_in(key, 404), grid_x * grid_y)
    chosen = jax.vmap(lambda item: jax.random.permutation(item, CX * CY * NZ)[:WALL])(keys)
    return chosen.reshape(grid_x, grid_y, WALL).astype(jnp.int32)


def draw_wall_count(key, part):
    grid_x = NX // CX
    grid_y = NY // CY
    shifted = jax.random.randint(jax.random.fold_in(key, 505), (grid_x, grid_y), 0, 4)
    counts = jnp.right_shift(jnp.full((grid_x, grid_y), WALL, jnp.int32), shifted.astype(jnp.int32))
    counts = jnp.maximum(counts, 1).at[0, 0].set(WALL)
    return counts.astype(jnp.int32)


def plant(result, rng, smallest, top_value):
    dims = result.shape
    spot = [jax.random.randint(jax.random.fold_in(rng, axis), (), 0, dims[axis]) for axis in range(len(dims))]
    result = result.at[tuple(spot)].set(smallest)
    longest = dims.index(max(dims))
    spot[longest] = (spot[longest] + 1) % dims[longest]
    return result.at[tuple(spot)].set(top_value)


def setup_inputs(seed: int = 0) -> dict:
    arg_keys = jax.random.split(jax.random.key(seed), 10)
    populations = draw_populations(jax.random.fold_in(arg_keys[9], 71), 0)
    relax = jnp.clip(jnp.exp(jax.random.uniform(arg_keys[1], (27,), jnp.float32, math.log(0.6), math.log(1.9))), 0.6, 1.9)
    solid = plant((jax.random.randint(arg_keys[2], (NX, NY, NZ), 0, 8) < 1).astype(jnp.int32), jax.random.fold_in(arg_keys[2], 1), 0, 1)
    wall_cell = draw_wall_cell(jax.random.fold_in(arg_keys[9], 71), 0)
    wall_normal = plant(jax.random.randint(arg_keys[4], (N_GX, N_GY, WALL), 0, 6), jax.random.fold_in(arg_keys[4], 1), 0, 5).astype(jnp.int32)
    wall_count = draw_wall_count(jax.random.fold_in(arg_keys[9], 71), 0)
    sample_ref = jax.vmap(lambda own: jax.random.permutation(own, WALL))(jax.random.split(arg_keys[6], N_GX * N_GY)).reshape((N_GX, N_GY, WALL)).astype(jnp.int32)
    stencil_cell = draw_stencil_cell(jax.random.fold_in(arg_keys[9], 71), 0)
    stencil_weight = draw_stencil_weight(jax.random.fold_in(arg_keys[9], 71), 0)
    return {"populations": populations, "relax": relax, "solid": solid, "wall_cell": wall_cell, "wall_normal": wall_normal, "wall_count": wall_count, "sample_ref": sample_ref, "stencil_cell": stencil_cell, "stencil_weight": stencil_weight}


lattice_steps = [(a - 1, b - 1, c - 1) for a in range(3) for b in range(3) for c in range(3)]
wall_ratio = (1.0 / 9.0) ** (1.0 / 7.0)


def lattice():
    steps = np.array(lattice_steps).T
    single = np.where(steps == 0, 2.0 / 3.0, 1.0 / 6.0)
    weights = np.prod(single, axis=0)
    vander = np.array([[1.0, 1.0, 1.0], [-1.0, 0.0, 1.0], [1.0, 0.0, 1.0]])
    undo = np.array([[0.0, -0.5, 0.5], [1.0, 0.0, -1.0], [0.0, 0.5, 0.5]])
    moment = np.kron(np.kron(vander, vander), vander)
    inverse = np.kron(np.kron(undo, undo), undo)
    return (jnp.asarray(steps, jnp.float32), jnp.asarray(weights, jnp.float32),
            jnp.asarray(moment, jnp.float32), jnp.asarray(inverse, jnp.float32))


def moments(pops):
    steps, weights, moment, inverse = lattice()
    scaled = weights[:, None] * pops
    density = jnp.sum(scaled, axis=0)
    momentum = jnp.dot(steps, scaled, precision=lax.Precision.HIGHEST)
    return density, momentum / density[None]


def equilibrium(density, velocity):
    steps, weights, moment, inverse = lattice()
    projected = jnp.dot(steps.T, velocity, precision=lax.Precision.HIGHEST)
    speed_sq = jnp.sum(velocity * velocity, axis=0)
    return density[None] * (1.0 + 3.0 * projected + 4.5 * projected * projected - 1.5 * speed_sq[None])


def collide(pops, relax):
    steps, weights, moment, inverse = lattice()
    scaled = weights[:, None] * pops
    density, velocity = moments(pops)
    balance = weights[:, None] * equilibrium(density, velocity)
    deviation = jnp.dot(moment, scaled - balance, precision=lax.Precision.HIGHEST) * relax[:, None]
    after = scaled - jnp.dot(inverse, deviation, precision=lax.Precision.HIGHEST)
    return after / weights[:, None]


def sample_velocity(velocity, corner_cells, corner_weight):
    picked = velocity[:, corner_cells]
    return jnp.sum(picked * corner_weight[None], axis=1)


def rebuild_columns(columns, density, velocity, normal, live, picked):
    axis_index = normal // 2
    sign = (2 * (normal % 2) - 1).astype(jnp.float32)
    normal_vec = (jnp.arange(3, dtype=jnp.int32)[:, None] == axis_index[None]).astype(jnp.float32) * sign[None]
    along = jnp.sum(picked * normal_vec, axis=0)
    tangential = picked - along[None] * normal_vec
    wall_eq = equilibrium(density, wall_ratio * tangential)
    local_eq = equilibrium(density, velocity)
    return jnp.where(live[None], wall_eq + columns - local_eq, columns)


def rebuild_block(block, density, velocity, cells, normal, live, picked):
    columns = rebuild_columns(block[:, cells], density[cells], velocity[:, cells], normal, live, picked)
    return block.at[:, cells].set(columns)


def to_blocks(field):
    count = field.shape[0]
    field = field.reshape(count, N_GX, CX, N_GY, CY, NZ).transpose(1, 3, 0, 2, 4, 5)
    return field.reshape(N_GX, N_GY, count, CX * CY * NZ)


def from_blocks(blocks):
    count = blocks.shape[2]
    field = blocks.reshape(N_GX, N_GY, count, CX, CY, NZ).transpose(2, 0, 3, 1, 4, 5)
    return field.reshape(count, N_GX * CX, N_GY * CY, NZ)


def reference(populations, relax, solid, wall_cell, wall_normal, wall_count, sample_ref, stencil_cell, stencil_weight):
    blocks = to_blocks(populations)
    density_b, velocity_b = lax.map(lambda row: jax.vmap(moments)(row), blocks)
    samples = jax.vmap(jax.vmap(sample_velocity))(velocity_b, stencil_cell, stencil_weight)
    sent = samples.reshape(N_GX, N_GY, 3, N_GY, SLOTS)
    received = sent.transpose(0, 3, 2, 1, 4).reshape(N_GX, N_GY, 3, N_GY * SLOTS)
    picked = jax.vmap(jax.vmap(lambda table, where_from: table[:, where_from]))(received, sample_ref)
    live = jnp.arange(N_GY * SLOTS, dtype=jnp.int32)[None, None, :] < wall_count[:, :, None]
    rebuilt = jax.vmap(jax.vmap(rebuild_block))(blocks, density_b, velocity_b, wall_cell, wall_normal, live, picked)
    post_b = lax.map(lambda row: jax.vmap(lambda block: collide(block, relax))(row), rebuilt)
    post = from_blocks(post_b)
    outputs = []
    for direction in range(27):
        step_x, step_y, step_z = lattice_steps[direction]
        moved = jnp.roll(post[direction], (step_x, step_y, step_z), axis=(0, 1, 2))
        blocked = jnp.roll(solid, (step_x, step_y, step_z), axis=(0, 1, 2))
        outputs.append(jnp.where(blocked != 0, post[26 - direction], moved))
    return jnp.stack(outputs)
```

```python
import functools

import jax
import jax.numpy as jnp
import numpy as np
from jax import lax
from jax.experimental import pallas as pl
from jax.experimental.pallas import tpu as pltpu
from jax.sharding import PartitionSpec as P

steps = np.array([(a - 1, b - 1, c - 1) for a in range(3) for b in range(3) for c in range(3)])
wall_ratio = (1.0 / 9.0) ** (1.0 / 7.0)
weights = np.prod(np.where(steps == 0, 2.0 / 3.0, 1.0 / 6.0), axis=1)
vander = np.array([[1.0, 1.0, 1.0], [-1.0, 0.0, 1.0], [1.0, 0.0, 1.0]])
moment = np.kron(np.kron(vander, vander), vander)
LANES = 128
MESH = pl.DeviceIdType.MESH


def equilibrium_moments():
    x, y, z = steps.T.astype(float)
    basis = np.stack(
        [
            np.ones(27),
            3 * x,
            3 * y,
            3 * z,
            4.5 * x * x - 1.5,
            4.5 * y * y - 1.5,
            4.5 * z * z - 1.5,
            9 * x * y,
            9 * x * z,
            9 * y * z,
        ],
        axis=1,
    )
    return moment @ (weights[:, None] * basis)


def forward(vals):
    for stride in (9, 3, 1):
        out = list(vals)
        for i in range(27):
            if i // stride % 3 == 0:
                lo, mid, hi = (vals[i], vals[i + stride], vals[i + 2 * stride])
                both = lo + hi
                out[i], out[i + stride], out[i + 2 * stride] = (both + mid, hi - lo, both)
        vals = out
    return vals


def plus(a, b):
    return b if a is None else a if b is None else a + b


def minus(a, b):
    return a if b is None else -b if a is None else a - b


def backward(vals):
    for stride in (9, 3, 1):
        out = list(vals)
        for i in range(27):
            if i // stride % 3 == 0:
                s0, s1, s2 = (vals[i], vals[i + stride], vals[i + 2 * stride])
                out[i], out[i + stride], out[i + 2 * stride] = (
                    minus(s2, s1),
                    minus(s0, s2),
                    plus(s2, s1),
                )
        vals = out
    return vals


def combine(terms):
    total = None
    for factor, value in terms:
        if abs(factor) < 1e-12:
            continue
        if abs(factor - 1.0) < 1e-12:
            total = plus(total, value)
        elif abs(factor + 1.0) < 1e-12:
            total = minus(total, value)
        else:
            total = plus(total, value * np.float32(factor))
    return total


def roll(value, shift, axis):
    return value if shift == 0 else pltpu.roll(value, shift % value.shape[axis], axis)


def lane_gather(row, index):
    return jnp.take_along_axis(
        jnp.broadcast_to(row, index.shape), index, axis=1, mode="promise_in_bounds"
    )


def kernel(
    devices_x,
    devices_y,
    pop_hbm,
    relax_hbm,
    solid_hbm,
    wall_hbm,
    normal_hbm,
    count_hbm,
    ref_hbm,
    stencil_hbm,
    weight_hbm,
    out,
    pop,
    relax,
    count,
    solid,
    lists,
    stencil,
    weight,
    vel,
    samples,
    rx_row,
    rx_x,
    post,
    settled,
    shifted,
    fields,
    face,
    near,
    corner,
    got_face,
    got_near,
    got_corner,
    lines,
    masks,
    moved,
    tally,
    load_sem,
    send_sem,
    near_sem,
    face_sem,
    far_sem,
):
    size_x, size_y = pop.shape[1:3]
    rows = size_x * size_y
    slots_all = lists.shape[2]
    slots = slots_all // devices_y
    shift_bits = slots.bit_length() - 1
    my_x = lax.axis_index("gx")
    my_y = lax.axis_index("gy")
    ratio = np.float32(wall_ratio)
    tile = (size_y, LANES)

    def wrap(value, size):
        return jnp.where(value < 0, value + size, jnp.where(value >= size, value - size, value))

    loads = [
        pltpu.make_async_copy(src, dst, load_sem.at[n])
        for n, src, dst in [
            (0, pop_hbm, pop),
            (1, stencil_hbm, stencil),
            (2, weight_hbm, weight),
            (3, wall_hbm.at[0], lists.at[0]),
            (3, normal_hbm.at[0], lists.at[1]),
            (3, ref_hbm.at[0], lists.at[2]),
            (4, count_hbm, count),
            (5, solid_hbm, solid),
            (6, relax_hbm, relax),
        ]
    ]
    for load in loads:
        load.start()
    barrier = pltpu.get_barrier_semaphore()
    columns = {dy: wrap(my_y + dy, devices_y) for dy in range(devices_y)}
    columns[-1] = columns[devices_y - 1]
    beside = {dx: wrap(my_x + dx, devices_x) for dx in (-1, 0, 1)}
    peers = [(dx, dy) for dx in (-1, 1, 0) for dy in range(devices_y) if (dx, dy) != (0, 0)]
    for dx, dy in peers:
        pl.semaphore_signal(
            barrier,
            inc=1,
            device_id={"gx": beside[dx], "gy": columns[dy]},
            device_id_type=MESH,
        )
    for n in (0, 1, 2):
        loads[n].wait()
    pltpu.make_async_copy(lists, lists, load_sem.at[3]).wait()
    for n in (6, 7, 8):
        loads[n].wait()

    row_line = lax.broadcasted_iota(jnp.int32, tile, 0)

    moments, speeds = ([], [])
    for x in range(size_x):
        found = forward([pop[i, x] * np.float32(weights[i]) for i in range(27)])
        rho = found[0]
        inverse = 1.0 / rho
        u = [found[9] * inverse, found[3] * inverse, found[1] * inverse]
        for c in range(3):
            vel[c * rows + x * size_y : c * rows + (x + 1) * size_y, :] = u[c]
        moments.append(found)
        speeds.append(u)

    cell = lists[0]
    slot = lax.broadcasted_iota(jnp.int32, (1, slots_all), 1)
    live = slot < count[0, 0]
    which = lists[2]
    row_hit = jnp.logical_and(
        lax.broadcasted_iota(jnp.int32, (rows, slots_all), 0) == jnp.right_shift(cell, 7), live
    )
    values = [
        jnp.right_shift(which, shift_bits) + 1,
        jnp.bitwise_and(which, slots - 1),
        jnp.right_shift(lists[1], 1),
    ]
    left = jnp.concatenate(
        [jnp.where(row_hit, value.astype(jnp.float32), 0.0) for value in values], axis=0
    ).astype(jnp.bfloat16)
    right = jnp.where(
        lax.broadcasted_iota(jnp.int32, (LANES, slots_all), 0)
        == jnp.bitwise_and(cell, LANES - 1),
        1.0,
        0.0,
    ).astype(jnp.bfloat16)
    table = lax.dot_general(
        left, right, (((1,), (1,)), ((), ())), preferred_element_type=jnp.float32
    )

    for part in range(slots_all // LANES):
        lanes = slice(part * LANES, (part + 1) * LANES)
        cells = stencil[0, 0, :, lanes]
        lane = jnp.bitwise_and(cells, LANES - 1)
        row = jnp.right_shift(cells, 7)
        picked = [jnp.zeros(cells.shape, jnp.float32)] * 3
        for r in range(rows):
            here = row == r
            for c in range(3):
                picked[c] = jnp.where(
                    here, lane_gather(vel[c * rows + r : c * rows + r + 1, :], lane), picked[c]
                )
        factor = weight[0, 0, :, lanes]
        for c in range(3):
            n = part * 3 + c
            samples[n : n + 1, :] = jnp.sum(picked[c] * factor, axis=0, keepdims=True)
    rx_row[my_y] = samples[...]

    def equilibrium_terms(n):
        square = [value * value for value in n]
        return 1.0 - 1.5 * (square[0] + square[1] + square[2])

    def along(n, step):
        total = None
        for c in range(3):
            if step[c] > 0:
                total = plus(total, n[c])
            elif step[c] < 0:
                total = minus(total, n[c])
        return total

    def pairs(rho, n):
        rest = rho * equilibrium_terms(n)
        found = {13: rest}
        rho3, rho45 = (rho * 3.0, rho * 4.5)
        for i in range(13):
            s = along(n, steps[i])
            even = rest + rho45 * s * s
            odd = rho3 * s
            found[i], found[26 - i] = (even + odd, even - odd)
        return found

    coefficient = equilibrium_moments()
    near_rows = [
        ((a + 1) * 3 + c + 1, x)
        for a in (-1, 0, 1)
        for c in (-1, 0, 1)
        for x in range(size_x)
        if 0 <= x + a < size_x
    ]
    ends = ((0, size_x - 1), (1, 0))
    for x in range(size_x):
        found, u = (moments[x], speeds[x])
        ux, uy, uz = u
        rho, mx, my, mz = (found[0], found[9], found[3], found[1])
        owner = table[x * size_y : (x + 1) * size_y]
        place = table[rows + x * size_y : rows + (x + 1) * size_y]
        axis = table[2 * rows + x * size_y : 2 * rows + (x + 1) * size_y]
        held = jnp.where(owner > 0.5, rho, 0.0)
        code = jnp.where(owner > 0.5, (owner - 1.0) * np.float32(slots) + place + 1.0, 0.0)
        marked = solid[x].astype(jnp.float32)
        extra = [held, code, axis, marked]
        for f in range(3):
            fields[f, x] = extra[f]
        basis = [rho, mx, my, mz, mx * ux, my * uy, mz * uz, mx * uy, mx * uz, my * uz]
        deviation = []
        for j in range(27):
            if j in (0, 1, 3, 9):
                deviation.append(None)
            else:
                balance = combine(list(zip(coefficient[j], basis)))
                deviation.append(minus(found[j], balance) * relax[j])
        change = backward(deviation)
        local = pairs(held, u)
        for i in range(27):
            a, b, c = steps[i]
            half = 0.5 ** int(np.sum(steps[i] != 0)) / weights[i]
            value = pop[i, x] - change[i] * np.float32(half) - local[i]
            post[i, x] = value
            for way, edge in ends:
                if x == edge and a == 1 - 2 * way:
                    face[way, (b + 1) * 3 + c + 1] = value
            if b != 0:
                side = 0 if b > 0 else 1
                y = size_y - 1 if b > 0 else 0
                line = value[y : y + 1, :]
                j = (a + 1) * 3 + c + 1
                if (j, x) in near_rows:
                    n = near_rows.index((j, x))
                    near[side, n : n + 1, :] = line
                else:
                    corner[0 if a > 0 else 1, side, c + 1 : c + 2, :] = line
        for way, edge in ends:
            if x == edge:
                for f in range(4):
                    face[way, 9 + f] = extra[f]
        for side, y in ((0, size_y - 1), (1, 0)):
            for f in range(4):
                line = extra[f][y : y + 1, :]
                n = len(near_rows) + f * size_x + x
                near[side, n : n + 1, :] = line
                for way, edge in ends:
                    if x == edge:
                        corner[way, side, 3 + f : 4 + f, :] = line

    def send(src, dst, sem, dx, dy):
        pltpu.make_async_remote_copy(
            src_ref=src,
            dst_ref=dst,
            send_sem=send_sem,
            recv_sem=sem,
            device_id={"gx": dx, "gy": columns[dy]},
            device_id_type=MESH,
        ).start()

    across = sorted(range(devices_y), key=lambda dy: -min(dy, devices_y - dy))
    pl.semaphore_wait(barrier, len(peers))
    first = jnp.where(my_x == 0, 1, 0)
    for step in range(2):
        way = first if step == 0 else 1 - first
        dx = wrap(my_x + 1 - 2 * way, devices_x)
        for dy in across:
            send(samples, rx_x.at[way, my_y], far_sem.at[way], dx, dy)
        for side, dy in ((0, 1), (1, -1)):
            send(corner.at[way, side], got_corner.at[way, side], far_sem.at[way], dx, dy)
        send(face.at[way], got_face.at[way], face_sem.at[way], dx, 0)
        if step == 0:
            for side, dy in ((0, 1), (1, -1)):
                send(near.at[side], got_near.at[side], near_sem, my_x, dy)
            for dy in across:
                if dy != 0:
                    send(samples, rx_row.at[my_y], near_sem, my_x, dy)

    def lookup(code, axis, operand, offset):
        r = code.astype(jnp.int32) - 1
        owner = jnp.right_shift(r, shift_bits)
        lane = jnp.bitwise_and(r, slots - 1) + offset
        value = [jnp.zeros(tile, jnp.float32)] * 3
        for peer in range(devices_y):
            here = owner == peer
            for c in range(3):
                value[c] = jnp.where(
                    here,
                    jnp.take_along_axis(operand(peer, c), lane, axis=1, mode="promise_in_bounds"),
                    value[c],
                )
        return [jnp.where(axis == np.float32(c), 0.0, value[c] * ratio) for c in range(3)]

    def spread(line):
        return jnp.broadcast_to(line, tile)

    def part_of(owner):
        return (owner * slots) // LANES * 3, lax.rem(owner * slots, LANES)

    def mend(value, line, b):
        edge = 0 if b > 0 else size_y - 1
        return jnp.where(row_line == edge, spread(line), value)

    part, offset = part_of(my_y)

    near_count = pltpu.make_async_copy(
        tally.at[0 : (2 * near.shape[1] + (devices_y - 1) * samples.shape[0]) // size_y],
        tally.at[0 : (2 * near.shape[1] + (devices_y - 1) * samples.shape[0]) // size_y],
        near_sem,
    )
    near_count.wait()
    for x in range(size_x):
        n = lookup(
            fields[1, x],
            fields[2, x],
            lambda peer, c: spread(rx_row[peer, pl.ds(part + c, 1), :]),
            offset,
        )
        found = pairs(fields[0, x], n)
        for i in range(27):
            _, b, c = steps[i]
            value = post[i, x] + found[i]
            settled[i, x] = value
            shifted[i, x] = roll(roll(value, b, 0), c, 1)

    for side in range(2):
        for n, (j, x) in enumerate(near_rows):
            q = side * size_x + x
            lines[j, q : q + 1, :] = got_near[side, n : n + 1, :]
        for f in range(4):
            for x in range(size_x):
                n = len(near_rows) + f * size_x + x
                q = side * size_x + x
                lines[9 + f, q : q + 1, :] = got_near[side, n : n + 1, :]
    lower = row_line < size_x
    part0, offset0 = part_of(columns[-1])
    part1, offset1 = part_of(columns[1])
    n = lookup(
        lines[10],
        lines[11],
        lambda peer, c: jnp.where(
            lower,
            spread(rx_row[peer, pl.ds(part0 + c, 1), :]),
            spread(rx_row[peer, pl.ds(part1 + c, 1), :]),
        ),
        jnp.where(lower, offset0, offset1),
    )
    sign_b = jnp.where(lower, 1.0, -1.0)
    n[1] = n[1] * sign_b
    rho = lines[9]
    rest = equilibrium_terms(n)
    border = []
    for j in range(9):
        a, c = (j // 3 - 1, j % 3 - 1)
        s = along(n, (a, 1, c))
        border.append(roll(lines[j] + rho * (rest + s * (3.0 + 4.5 * s)), c, 1))
    marked = [roll(lines[12], c, 1) for c in (-1, 0, 1)]
    for x in range(size_x):
        plane = solid[x].astype(jnp.float32)
        for b in (-1, 0, 1):
            turned = roll(plane, b, 0)
            for c in (-1, 0, 1):
                value = roll(turned, c, 1)
                if b != 0:
                    q = (0 if b > 0 else 1) * size_x + x
                    value = mend(value, marked[c + 1][q : q + 1, :], b)
                masks[(b + 1) * 3 + c + 1, x] = value
    for i in range(27):
        a, b, c = steps[i]
        k = (b + 1) * 3 + c + 1
        for x in range(size_x):
            origin = x - a
            if 0 <= origin < size_x:
                value = shifted[i, origin]
                if b != 0:
                    q = (0 if b > 0 else 1) * size_x + origin
                    value = mend(value, border[(a + 1) * 3 + c + 1][q : q + 1, :], b)
                out[i, x] = jnp.where(masks[k, origin] != 0, settled[26 - i, x], value)

    for way in (1, 0):
        pltpu.make_async_copy(got_face.at[way], got_face.at[way], face_sem.at[way]).wait()
        for k in range(9):
            b, c = (k // 3 - 1, k % 3 - 1)
            moved[way, k] = roll(roll(got_face[way, k], b, 0), c, 1)
            moved[way, 9 + k] = roll(roll(got_face[way, 12], b, 0), c, 1)

    far_tiles = (devices_y * samples.shape[0] + 2 * corner.shape[2]) // size_y
    for way in (1, 0):
        pltpu.make_async_copy(
            tally.at[0:far_tiles], tally.at[0:far_tiles], far_sem.at[way]
        ).wait()

    def stack(line):
        return jnp.where(
            row_line == 0,
            spread(line(0, 0)),
            jnp.where(
                row_line == 1,
                spread(line(0, 1)),
                jnp.where(row_line == 2, spread(line(1, 0)), spread(line(1, 1))),
            ),
        )

    quantity = [stack(lambda way, side: got_corner[way, side, f : f + 1, :]) for f in range(7)]
    even = jnp.bitwise_and(row_line, 1) == 0
    parts = (part0, part1)
    n = lookup(
        quantity[4],
        quantity[5],
        lambda peer, c: stack(lambda way, side: rx_x[way, peer, pl.ds(parts[side] + c, 1), :]),
        jnp.where(even, offset0, offset1),
    )
    rest = equilibrium_terms(n)
    s = jnp.where(row_line < 2, n[0], -n[0]) + jnp.where(even, n[1], -n[1])
    corners, marked = ([], [])
    for c in (-1, 0, 1):
        t = s if c == 0 else s + n[2] if c > 0 else s - n[2]
        value = quantity[c + 1] + quantity[3] * (rest + t * (3.0 + 4.5 * t))
        corners.append(roll(value, c, 1))
        marked.append(roll(quantity[6], c, 1))

    for way, a in ((1, -1), (0, 1)):
        n = lookup(
            got_face[way, 10],
            got_face[way, 11],
            lambda peer, c: spread(rx_x[way, peer, pl.ds(part + c, 1), :]),
            offset,
        )
        rho = got_face[way, 9]
        rest = equilibrium_terms(n)
        x = 0 if a > 0 else size_x - 1
        for k in range(9):
            b, c = (k // 3 - 1, k % 3 - 1)
            i = (a + 1) * 9 + k
            s = along(n, (a, b, c))
            value = moved[way, k] + roll(roll(rho * (rest + s * (3.0 + 4.5 * s)), b, 0), c, 1)
            mark = moved[way, 9 + k]
            if b != 0:
                q = way * 2 + (0 if b > 0 else 1)
                value = mend(value, corners[c + 1][q : q + 1, :], b)
                mark = mend(mark, marked[c + 1][q : q + 1, :], b)
            out[i, x] = jnp.where(mark != 0, settled[26 - i, x], value)
    pltpu.make_async_copy(tally, tally, send_sem).wait()


def write_out(source, out, sem):
    copy = pltpu.make_async_copy(source, out, sem)
    copy.start()
    copy.wait()


def local(populations, relax, solid, wall_cell, wall_normal, wall_count, sample_ref, cells, factors):
    devices_x, devices_y = (lax.axis_size("gx"), lax.axis_size("gy"))
    size_x, size_y, size_z = populations.shape[1:]
    slots_all = wall_cell.shape[2]
    slots = slots_all // devices_y
    assert size_z == LANES and LANES % slots == 0 and slots & (slots - 1) == 0
    assert slots_all % LANES == 0 and devices_x > 2 and devices_y > 2
    assert 1 < size_x and 2 * size_x <= size_y == 8
    f32, i32 = (jnp.float32, jnp.int32)
    near_lines = -(-(9 * size_x - 6 + 4 * size_x) // 8) * 8
    held = -(-3 * slots_all // LANES // 8) * 8
    sent = (3 * devices_y - 1) * held + 2 * 13 * size_y + 2 * near_lines + 4 * 8
    vmem = pltpu.VMEM
    tile = (size_y, LANES)
    anywhere = pl.BlockSpec(memory_space=pl.ANY)
    dma = pltpu.SemaphoreType.DMA
    result = pl.pallas_call(
        functools.partial(kernel, devices_x, devices_y),
        out_shape=pltpu.VMEM(populations.shape, f32),
        in_specs=[anywhere] * 9,
        out_specs=pl.BlockSpec(memory_space=pltpu.VMEM),
        scratch_shapes=[
            vmem(populations.shape, f32),
            pltpu.SMEM(relax.shape, f32),
            pltpu.SMEM(wall_count.shape, i32),
            vmem(solid.shape, i32),
            vmem((3, 1, slots_all), i32),
            vmem(cells.shape, i32),
            vmem(factors.shape, f32),
            vmem((3 * size_x * size_y, LANES), f32),
            vmem((held, LANES), f32),
            vmem((devices_y, held, LANES), f32),
            vmem((2, devices_y, held, LANES), f32),
            vmem(populations.shape, f32),
            vmem(populations.shape, f32),
            vmem(populations.shape, f32),
            vmem((3, size_x) + tile, f32),
            vmem((2, 13) + tile, f32),
            vmem((2, near_lines, LANES), f32),
            vmem((2, 2, 8, LANES), f32),
            vmem((2, 13) + tile, f32),
            vmem((2, near_lines, LANES), f32),
            vmem((2, 2, 8, LANES), f32),
            vmem((13,) + tile, f32),
            vmem((9, size_x) + tile, f32),
            vmem((2, 18) + tile, f32),
            vmem((sent // size_y,) + tile, f32),
            dma((7,)),
            dma,
            dma,
            dma((2,)),
            dma((2,)),
        ],
        compiler_params=pltpu.CompilerParams(collective_id=0, has_side_effects=True),
        name="lattice_step",
    )(populations, relax, solid, wall_cell, wall_normal, wall_count, sample_ref, cells, factors)
    result = pltpu.with_memory_space_constraint(result, pltpu.VMEM)
    return pl.pallas_call(
        write_out,
        out_shape=jax.ShapeDtypeStruct(populations.shape, f32),
        in_specs=[pl.BlockSpec(memory_space=pltpu.VMEM)],
        out_specs=anywhere,
        scratch_shapes=[pltpu.SemaphoreType.DMA],
        name="write_out",
    )(result)


def solution(mesh):
    return jax.shard_map(
        local,
        mesh=mesh,
        in_specs=(
            P(None, "gx", "gy", None),
            P(),
            P("gx", "gy", None),
            P("gx", "gy", None),
            P("gx", "gy", None),
            P("gx", "gy"),
            P("gx", "gy", None),
            P("gx", "gy", None, None),
            P("gx", "gy", None, None),
        ),
        out_specs=P(None, "gx", "gy", None),
        check_vma=False,
    )
```

```python
import functools

import jax
import jax.numpy as jnp
import numpy as np
from jax import lax
from jax.experimental import pallas as pl
from jax.experimental.pallas import tpu as pltpu
from jax.sharding import PartitionSpec as P


steps = np.array([(a - 1, b - 1, c - 1) for a in range(3) for b in range(3) for c in range(3)])
wall_ratio = (1.0 / 9.0) ** (1.0 / 7.0)
weights = np.prod(np.where(steps == 0, 2.0 / 3.0, 1.0 / 6.0), axis=1)
vander = np.array([[1.0, 1.0, 1.0], [-1.0, 0.0, 1.0], [1.0, 0.0, 1.0]])
moment = np.kron(np.kron(vander, vander), vander)
LANES = 128
MESH = pl.DeviceIdType.MESH


def equilibrium_moments():
    x, y, z = steps.T.astype(float)
    basis = np.stack(
        [
            np.ones(27),
            3 * x,
            3 * y,
            3 * z,
            4.5 * x * x - 1.5,
            4.5 * y * y - 1.5,
            4.5 * z * z - 1.5,
            9 * x * y,
            9 * x * z,
            9 * y * z,
        ],
        axis=1,
    )
    return moment @ (weights[:, None] * basis)


def forward(vals):
    for stride in (9, 3, 1):
        out = list(vals)
        for i in range(27):
            if i // stride % 3 == 0:
                lo, mid, hi = (vals[i], vals[i + stride], vals[i + 2 * stride])
                both = lo + hi
                out[i], out[i + stride], out[i + 2 * stride] = (both + mid, hi - lo, both)
        vals = out
    return vals


def plus(a, b):
    return b if a is None else a if b is None else a + b


def minus(a, b):
    return a if b is None else -b if a is None else a - b


def backward(vals):
    for stride in (9, 3, 1):
        out = list(vals)
        for i in range(27):
            if i // stride % 3 == 0:
                s0, s1, s2 = (vals[i], vals[i + stride], vals[i + 2 * stride])
                out[i], out[i + stride], out[i + 2 * stride] = (
                    minus(s2, s1),
                    minus(s0, s2),
                    plus(s2, s1),
                )
        vals = out
    return vals


def combine(terms):
    total = None
    for factor, value in terms:
        if abs(factor) < 1e-12:
            continue
        if abs(factor - 1.0) < 1e-12:
            total = plus(total, value)
        elif abs(factor + 1.0) < 1e-12:
            total = minus(total, value)
        else:
            total = plus(total, value * np.float32(factor))
    return total


def roll(value, shift, axis):
    return value if shift == 0 else pltpu.roll(value, shift % value.shape[axis], axis)


def lane_gather(row, index):
    return jnp.take_along_axis(
        jnp.broadcast_to(row, index.shape), index, axis=1, mode="promise_in_bounds"
    )


def kernel(
    devices_x,
    devices_y,
    gate,
    pop,
    relax,
    solid,
    wall,
    normal,
    count,
    ref,
    stencil,
    weight,
    out,
    vel,
    samples,
    rx_row,
    rx_x,
    post,
    settled,
    shifted,
    fields,
    face,
    near,
    corner,
    got_face,
    got_near,
    got_corner,
    lines,
    masks,
    moved,
    tally,
    send_sem,
    near_sem,
    face_sem,
    far_sem,
    row_ready,
    ready,
):
    size_x, size_y = pop.shape[1:3]
    rows = size_x * size_y
    slots_all = wall.shape[2]
    slots = slots_all // devices_y
    shift_bits = slots.bit_length() - 1
    my_x = lax.axis_index("gx")
    my_y = lax.axis_index("gy")
    ratio = np.float32(wall_ratio)
    tile = (size_y, LANES)

    def wrap(value, size):
        return jnp.where(value < 0, value + size, jnp.where(value >= size, value - size, value))

    barrier = pltpu.get_barrier_semaphore()
    columns = {dy: wrap(my_y + dy, devices_y) for dy in range(devices_y)}
    columns[-1] = columns[devices_y - 1]
    beside = {dx: wrap(my_x + dx, devices_x) for dx in (-1, 0, 1)}
    last = devices_x - 1
    inner = my_y - jnp.bitwise_and(my_y, 1)
    outer = inner + 2
    below = jnp.minimum(outer, devices_y)

    def tell(sem, dx, dy):
        pl.semaphore_signal(
            sem,
            inc=1,
            device_id={"gx": beside[dx], "gy": columns[dy]},
            device_id_type=MESH,
        )

    def when(condition, *signal):
        pl.when(condition)(lambda: tell(*signal))

    at_last = my_x == last
    inward = jnp.where(my_x == 0, inner, 0)
    outward = jnp.where(at_last, devices_y, jnp.where(my_x == last - 1, inner, 0))
    higher = jnp.where(at_last, devices_y, 2 * devices_y)
    for dy in range(devices_y):
        when(columns[dy] >= inward, barrier, -1, dy)
    for dy in range(devices_y):
        when(columns[dy] >= outward, barrier, 1, dy)
    for dy in range(1, devices_y):
        when(my_y + dy < higher, barrier, 0, dy)

    row_line = lax.broadcasted_iota(jnp.int32, tile, 0)

    moments, speeds = ([], [])
    for x in range(size_x):
        found = forward([pop[i, x] * np.float32(weights[i]) for i in range(27)])
        rho = found[0]
        inverse = 1.0 / rho
        u = [found[9] * inverse, found[3] * inverse, found[1] * inverse]
        for c in range(3):
            vel[c * rows + x * size_y : c * rows + (x + 1) * size_y, :] = u[c]
        moments.append(found)
        speeds.append(u)

    cell = wall[0]
    slot = lax.broadcasted_iota(jnp.int32, (1, slots_all), 1)
    live = slot < count[0, 0]
    which = ref[0]
    row_hit = jnp.logical_and(
        lax.broadcasted_iota(jnp.int32, (rows, slots_all), 0) == jnp.right_shift(cell, 7), live
    )
    values = [
        jnp.right_shift(which, shift_bits) + 1,
        jnp.bitwise_and(which, slots - 1),
        jnp.right_shift(normal[0], 1),
    ]
    left = jnp.concatenate(
        [jnp.where(row_hit, value.astype(jnp.float32), 0.0) for value in values], axis=0
    ).astype(jnp.bfloat16)
    right = jnp.where(
        lax.broadcasted_iota(jnp.int32, (LANES, slots_all), 0)
        == jnp.bitwise_and(cell, LANES - 1),
        1.0,
        0.0,
    ).astype(jnp.bfloat16)
    table = lax.dot_general(
        left, right, (((1,), (1,)), ((), ())), preferred_element_type=jnp.float32
    )

    for part in range(slots_all // LANES):
        lanes = slice(part * LANES, (part + 1) * LANES)
        cells = stencil[0, 0, :, lanes]
        lane = jnp.bitwise_and(cells, LANES - 1)
        row = jnp.right_shift(cells, 7)
        picked = [jnp.zeros(cells.shape, jnp.float32)] * 3
        for r in range(rows):
            here = row == r
            for c in range(3):
                picked[c] = jnp.where(
                    here, lane_gather(vel[c * rows + r : c * rows + r + 1, :], lane), picked[c]
                )
        factor = weight[0, 0, :, lanes]
        for c in range(3):
            n = part * 3 + c
            samples[n : n + 1, :] = jnp.sum(picked[c] * factor, axis=0, keepdims=True)
    rx_row[my_y] = samples[...]

    def equilibrium_terms(n):
        square = [value * value for value in n]
        return 1.0 - 1.5 * (square[0] + square[1] + square[2])

    def along(n, step):
        total = None
        for c in range(3):
            if step[c] > 0:
                total = plus(total, n[c])
            elif step[c] < 0:
                total = minus(total, n[c])
        return total

    def pairs(rho, n):
        rest = rho * equilibrium_terms(n)
        found = {13: rest}
        rho3, rho45 = (rho * 3.0, rho * 4.5)
        for i in range(13):
            s = along(n, steps[i])
            even = rest + rho45 * s * s
            odd = rho3 * s
            found[i], found[26 - i] = (even + odd, even - odd)
        return found

    coefficient = equilibrium_moments()
    rates = [jnp.broadcast_to(relax[0:1, j : j + 1], tile) for j in range(27)]
    near_rows = [
        ((a + 1) * 3 + c + 1, x)
        for a in (-1, 0, 1)
        for c in (-1, 0, 1)
        for x in range(size_x)
        if 0 <= x + a < size_x
    ]
    ends = ((0, size_x - 1), (1, 0))
    for x in range(size_x):
        found, u = (moments[x], speeds[x])
        ux, uy, uz = u
        rho, mx, my, mz = (found[0], found[9], found[3], found[1])
        owner = table[x * size_y : (x + 1) * size_y]
        place = table[rows + x * size_y : rows + (x + 1) * size_y]
        axis = table[2 * rows + x * size_y : 2 * rows + (x + 1) * size_y]
        held = jnp.where(owner > 0.5, rho, 0.0)
        code = jnp.where(owner > 0.5, (owner - 1.0) * np.float32(slots) + place + 1.0, 0.0)
        marked = solid[x].astype(jnp.float32)
        extra = [held, code, axis, marked]
        for f in range(3):
            fields[f, x] = extra[f]
        basis = [rho, mx, my, mz, mx * ux, my * uy, mz * uz, mx * uy, mx * uz, my * uz]
        deviation = []
        for j in range(27):
            if j in (0, 1, 3, 9):
                deviation.append(None)
            else:
                balance = combine(list(zip(coefficient[j], basis)))
                deviation.append(minus(found[j], balance) * rates[j])
        change = backward(deviation)
        local = pairs(held, u)
        for i in range(27):
            a, b, c = steps[i]
            half = 0.5 ** int(np.sum(steps[i] != 0)) / weights[i]
            value = pop[i, x] - change[i] * np.float32(half) - local[i]
            post[i, x] = value
            for way, edge in ends:
                if x == edge and a == 1 - 2 * way:
                    face[way, (b + 1) * 3 + c + 1] = value
            if b != 0:
                side = 0 if b > 0 else 1
                y = size_y - 1 if b > 0 else 0
                line = value[y : y + 1, :]
                j = (a + 1) * 3 + c + 1
                if (j, x) in near_rows:
                    n = near_rows.index((j, x))
                    near[side, n : n + 1, :] = line
                else:
                    corner[0 if a > 0 else 1, side, c + 1 : c + 2, :] = line
        for way, edge in ends:
            if x == edge:
                for f in range(4):
                    face[way, 9 + f] = extra[f]
        for side, y in ((0, size_y - 1), (1, 0)):
            for f in range(4):
                line = extra[f][y : y + 1, :]
                n = len(near_rows) + f * size_x + x
                near[side, n : n + 1, :] = line
                for way, edge in ends:
                    if x == edge:
                        corner[way, side, 3 + f : 4 + f, :] = line

    def send(src, dst, sem, dx, dy):
        pltpu.make_async_remote_copy(
            src_ref=src,
            dst_ref=dst,
            send_sem=send_sem,
            recv_sem=sem,
            device_id={"gx": dx, "gy": columns[dy]},
            device_id_type=MESH,
        ).start()

    across = sorted(range(devices_y), key=lambda dy: -min(dy, devices_y - dy))

    def send_to(way, dy):
        dx = beside[1 - 2 * way]
        send(samples, rx_x.at[way, my_y], far_sem.at[way], dx, dy)
        for side, corner_dy in ((0, 1), (1, devices_y - 1)):
            if dy == corner_dy:
                send(corner.at[way, side], got_corner.at[way, side], far_sem.at[way], dx, dy)
        if dy == 0:
            send(face.at[way], got_face.at[way], face_sem.at[way], dx, dy)

    def send_all(way):
        for dy in across:
            send_to(way, dy)

    known = (3 * devices_y - 1) - jnp.where(my_x == 0, devices_y, 0)
    pl.semaphore_wait(barrier, jnp.where(at_last, my_y + 2 * below, known))
    answer = jnp.where(at_last, outer, jnp.where(my_x == last - 1, inner, 0))
    for dy in across:
        when(columns[dy] < answer, ready, 1, dy)

    def expect(sem, amount):
        pl.when(amount > 0)(lambda: pl.semaphore_wait(sem, amount))

    def send_near():
        for side, dy in ((0, 1), (1, -1)):
            send(near.at[side], got_near.at[side], near_sem, my_x, dy)
        for dy in across:
            if dy != 0:
                send(samples, rx_row.at[my_y], near_sem, my_x, dy)

    @pl.when(at_last)
    def _():
        for dy in across:
            pl.when(columns[dy] < outer)(lambda dy=dy: send_to(0, dy))
        for dy in range(1, devices_y):
            when(my_y + dy >= devices_y, row_ready, 0, dy)
        expect(row_ready, devices_y - 1 - my_y)
        for dy in across:

            @pl.when(columns[dy] >= outer)
            def _(dy=dy):
                tell(ready, 1, dy)
                send_to(0, dy)

        send_near()
        expect(ready, devices_y - below)
        send_all(1)

    @pl.when(my_x < last)
    def _():
        send_near()
        send_all(0)

        @pl.when(my_x > 0)
        def _():
            send_all(1)

    def lookup(code, axis, operand, offset):
        r = code.astype(jnp.int32) - 1
        owner = jnp.right_shift(r, shift_bits)
        lane = jnp.bitwise_and(r, slots - 1) + offset
        value = [jnp.zeros(tile, jnp.float32)] * 3
        for peer in range(devices_y):
            here = owner == peer
            for c in range(3):
                value[c] = jnp.where(
                    here,
                    jnp.take_along_axis(operand(peer, c), lane, axis=1, mode="promise_in_bounds"),
                    value[c],
                )
        return [jnp.where(axis == np.float32(c), 0.0, value[c] * ratio) for c in range(3)]

    def spread(line):
        return jnp.broadcast_to(line, tile)

    def part_of(owner):
        return (owner * slots) // LANES * 3, lax.rem(owner * slots, LANES)

    def mend(value, line, b):
        edge = 0 if b > 0 else size_y - 1
        return jnp.where(row_line == edge, spread(line), value)

    part, offset = part_of(my_y)

    near_count = pltpu.make_async_copy(
        tally.at[0 : (2 * near.shape[1] + (devices_y - 1) * samples.shape[0]) // size_y],
        tally.at[0 : (2 * near.shape[1] + (devices_y - 1) * samples.shape[0]) // size_y],
        near_sem,
    )
    near_count.wait()
    for x in range(size_x):
        n = lookup(
            fields[1, x],
            fields[2, x],
            lambda peer, c: spread(rx_row[peer, pl.ds(part + c, 1), :]),
            offset,
        )
        found = pairs(fields[0, x], n)
        for i in range(27):
            _, b, c = steps[i]
            value = post[i, x] + found[i]
            settled[i, x] = value
            shifted[i, x] = roll(roll(value, b, 0), c, 1)

    for side in range(2):
        for n, (j, x) in enumerate(near_rows):
            q = side * size_x + x
            lines[j, q : q + 1, :] = got_near[side, n : n + 1, :]
        for f in range(4):
            for x in range(size_x):
                n = len(near_rows) + f * size_x + x
                q = side * size_x + x
                lines[9 + f, q : q + 1, :] = got_near[side, n : n + 1, :]
    lower = row_line < size_x
    part0, offset0 = part_of(columns[-1])
    part1, offset1 = part_of(columns[1])
    n = lookup(
        lines[10],
        lines[11],
        lambda peer, c: jnp.where(
            lower,
            spread(rx_row[peer, pl.ds(part0 + c, 1), :]),
            spread(rx_row[peer, pl.ds(part1 + c, 1), :]),
        ),
        jnp.where(lower, offset0, offset1),
    )
    sign_b = jnp.where(lower, 1.0, -1.0)
    n[1] = n[1] * sign_b
    rho = lines[9]
    rest = equilibrium_terms(n)
    border = []
    for j in range(9):
        a, c = (j // 3 - 1, j % 3 - 1)
        s = along(n, (a, 1, c))
        border.append(roll(lines[j] + rho * (rest + s * (3.0 + 4.5 * s)), c, 1))
    marked = [roll(lines[12], c, 1) for c in (-1, 0, 1)]
    for x in range(size_x):
        plane = solid[x].astype(jnp.float32)
        for b in (-1, 0, 1):
            turned = roll(plane, b, 0)
            for c in (-1, 0, 1):
                value = roll(turned, c, 1)
                if b != 0:
                    q = (0 if b > 0 else 1) * size_x + x
                    value = mend(value, marked[c + 1][q : q + 1, :], b)
                masks[(b + 1) * 3 + c + 1, x] = value
    for i in range(27):
        a, b, c = steps[i]
        k = (b + 1) * 3 + c + 1
        for x in range(size_x):
            origin = x - a
            if 0 <= origin < size_x:
                value = shifted[i, origin]
                if b != 0:
                    q = (0 if b > 0 else 1) * size_x + origin
                    value = mend(value, border[(a + 1) * 3 + c + 1][q : q + 1, :], b)
                out[i, x] = jnp.where(masks[k, origin] != 0, settled[26 - i, x], value)

    @pl.when(my_x == 0)
    def _():
        pl.semaphore_wait(ready, devices_y)
        send_all(1)

    for way in (1, 0):
        pltpu.make_async_copy(got_face.at[way], got_face.at[way], face_sem.at[way]).wait()
        for k in range(9):
            b, c = (k // 3 - 1, k % 3 - 1)
            moved[way, k] = roll(roll(got_face[way, k], b, 0), c, 1)
            moved[way, 9 + k] = roll(roll(got_face[way, 12], b, 0), c, 1)

    far_tiles = (devices_y * samples.shape[0] + 2 * corner.shape[2]) // size_y
    for way in (1, 0):
        pltpu.make_async_copy(
            tally.at[0:far_tiles], tally.at[0:far_tiles], far_sem.at[way]
        ).wait()

    def stack(line):
        return jnp.where(
            row_line == 0,
            spread(line(0, 0)),
            jnp.where(
                row_line == 1,
                spread(line(0, 1)),
                jnp.where(row_line == 2, spread(line(1, 0)), spread(line(1, 1))),
            ),
        )

    quantity = [stack(lambda way, side: got_corner[way, side, f : f + 1, :]) for f in range(7)]
    even = jnp.bitwise_and(row_line, 1) == 0
    parts = (part0, part1)
    n = lookup(
        quantity[4],
        quantity[5],
        lambda peer, c: stack(lambda way, side: rx_x[way, peer, pl.ds(parts[side] + c, 1), :]),
        jnp.where(even, offset0, offset1),
    )
    rest = equilibrium_terms(n)
    s = jnp.where(row_line < 2, n[0], -n[0]) + jnp.where(even, n[1], -n[1])
    corners, marked = ([], [])
    for c in (-1, 0, 1):
        t = s if c == 0 else s + n[2] if c > 0 else s - n[2]
        value = quantity[c + 1] + quantity[3] * (rest + t * (3.0 + 4.5 * t))
        corners.append(roll(value, c, 1))
        marked.append(roll(quantity[6], c, 1))

    for way, a in ((1, -1), (0, 1)):
        n = lookup(
            got_face[way, 10],
            got_face[way, 11],
            lambda peer, c: spread(rx_x[way, peer, pl.ds(part + c, 1), :]),
            offset,
        )
        rho = got_face[way, 9]
        rest = equilibrium_terms(n)
        x = 0 if a > 0 else size_x - 1
        for k in range(9):
            b, c = (k // 3 - 1, k % 3 - 1)
            i = (a + 1) * 9 + k
            s = along(n, (a, b, c))
            value = moved[way, k] + roll(roll(rho * (rest + s * (3.0 + 4.5 * s)), b, 0), c, 1)
            mark = moved[way, 9 + k]
            if b != 0:
                q = way * 2 + (0 if b > 0 else 1)
                value = mend(value, corners[c + 1][q : q + 1, :], b)
                mark = mend(mark, marked[c + 1][q : q + 1, :], b)
            out[i, x] = jnp.where(mark != 0, settled[26 - i, x], value)
    pltpu.make_async_copy(tally, tally, send_sem).wait()


def write_out(source, out, sem):
    copy = pltpu.make_async_copy(source, out, sem)
    copy.start()
    copy.wait()


def pause(out):
    out[...] = jnp.zeros_like(out)


def local(populations, relax, solid, wall_cell, wall_normal, wall_count, sample_ref, cells, factors):
    devices_x, devices_y = (lax.axis_size("gx"), lax.axis_size("gy"))
    size_x, size_y, size_z = populations.shape[1:]
    slots_all = wall_cell.shape[2]
    slots = slots_all // devices_y
    assert size_z == LANES and LANES % slots == 0 and slots & (slots - 1) == 0
    assert slots_all % LANES == 0 and devices_x > 2 and devices_y > 2
    assert 1 < size_x and 2 * size_x <= size_y == 8
    f32 = jnp.float32
    near_lines = -(-(9 * size_x - 6 + 4 * size_x) // 8) * 8
    held = -(-3 * slots_all // LANES // 8) * 8
    sent = (3 * devices_y - 1) * held + 2 * 13 * size_y + 2 * near_lines + 4 * 8
    vmem = pltpu.VMEM
    tile = (size_y, LANES)
    anywhere = pl.BlockSpec(memory_space=pl.ANY)
    on_core = pl.BlockSpec(memory_space=pltpu.VMEM)
    scalars = pl.BlockSpec(memory_space=pltpu.SMEM)

    def near_core(value):
        return pltpu.with_memory_space_constraint(value, pltpu.VMEM)

    dma = pltpu.SemaphoreType.DMA
    regular = pltpu.SemaphoreType.REGULAR
    gate = pl.pallas_call(
        pause,
        out_shape=pltpu.VMEM(tile, f32),
        out_specs=pl.BlockSpec(memory_space=pltpu.VMEM),
        cost_estimate=pl.CostEstimate(flops=10**9, bytes_accessed=4096, transcendentals=0),
        name="pause",
    )()
    result = pl.pallas_call(
        functools.partial(kernel, devices_x, devices_y),
        out_shape=pltpu.VMEM(populations.shape, f32),
        in_specs=[on_core] * 6 + [scalars] + [on_core] * 3,
        out_specs=pl.BlockSpec(memory_space=pltpu.VMEM),
        scratch_shapes=[
            vmem((3 * size_x * size_y, LANES), f32),
            vmem((held, LANES), f32),
            vmem((devices_y, held, LANES), f32),
            vmem((2, devices_y, held, LANES), f32),
            vmem(populations.shape, f32),
            vmem(populations.shape, f32),
            vmem(populations.shape, f32),
            vmem((3, size_x) + tile, f32),
            vmem((2, 13) + tile, f32),
            vmem((2, near_lines, LANES), f32),
            vmem((2, 2, 8, LANES), f32),
            vmem((2, 13) + tile, f32),
            vmem((2, near_lines, LANES), f32),
            vmem((2, 2, 8, LANES), f32),
            vmem((13,) + tile, f32),
            vmem((9, size_x) + tile, f32),
            vmem((2, 18) + tile, f32),
            vmem((sent // size_y,) + tile, f32),
            dma,
            dma,
            dma((2,)),
            dma((2,)),
            regular,
            regular,
        ],
        compiler_params=pltpu.CompilerParams(collective_id=0, has_side_effects=True),
        name="lattice_step",
    )(
        pltpu.with_memory_space_constraint(gate, pltpu.VMEM),
        near_core(populations),
        near_core(relax.reshape(1, 27)),
        near_core(solid),
        near_core(wall_cell),
        near_core(wall_normal),
        wall_count,
        near_core(sample_ref),
        near_core(cells),
        near_core(factors),
    )
    result = pltpu.with_memory_space_constraint(result, pltpu.VMEM)
    return pl.pallas_call(
        write_out,
        out_shape=jax.ShapeDtypeStruct(populations.shape, f32),
        in_specs=[pl.BlockSpec(memory_space=pltpu.VMEM)],
        out_specs=anywhere,
        scratch_shapes=[pltpu.SemaphoreType.DMA],
        name="write_out",
    )(result)


def solution(mesh):
    return jax.shard_map(
        local,
        mesh=mesh,
        in_specs=(
            P(None, "gx", "gy", None),
            P(),
            P("gx", "gy", None),
            P("gx", "gy", None),
            P("gx", "gy", None),
            P("gx", "gy"),
            P("gx", "gy", None),
            P("gx", "gy", None, None),
            P("gx", "gy", None, None),
        ),
        out_specs=P(None, "gx", "gy", None),
        check_vma=False,
    )
```

```python
import functools

import jax
import jax.numpy as jnp
import numpy as np
from jax import lax
from jax.experimental import pallas as pl
from jax.experimental.pallas import tpu as pltpu
from jax.sharding import PartitionSpec as P


steps = np.array([(a - 1, b - 1, c - 1) for a in range(3) for b in range(3) for c in range(3)])
wall_ratio = (1.0 / 9.0) ** (1.0 / 7.0)
weights = np.prod(np.where(steps == 0, 2.0 / 3.0, 1.0 / 6.0), axis=1)
vander = np.array([[1.0, 1.0, 1.0], [-1.0, 0.0, 1.0], [1.0, 0.0, 1.0]])
moment = np.kron(np.kron(vander, vander), vander)
LANES = 128
MESH = pl.DeviceIdType.MESH


def equilibrium_moments():
    x, y, z = steps.T.astype(float)
    basis = np.stack(
        [
            np.ones(27),
            3 * x,
            3 * y,
            3 * z,
            4.5 * x * x - 1.5,
            4.5 * y * y - 1.5,
            4.5 * z * z - 1.5,
            9 * x * y,
            9 * x * z,
            9 * y * z,
        ],
        axis=1,
    )
    return moment @ (weights[:, None] * basis)


def forward(vals):
    for stride in (9, 3, 1):
        out = list(vals)
        for i in range(27):
            if i // stride % 3 == 0:
                lo, mid, hi = (vals[i], vals[i + stride], vals[i + 2 * stride])
                both = lo + hi
                out[i], out[i + stride], out[i + 2 * stride] = (both + mid, hi - lo, both)
        vals = out
    return vals


def plus(a, b):
    return b if a is None else a if b is None else a + b


def minus(a, b):
    return a if b is None else -b if a is None else a - b


def backward(vals):
    for stride in (9, 3, 1):
        out = list(vals)
        for i in range(27):
            if i // stride % 3 == 0:
                s0, s1, s2 = (vals[i], vals[i + stride], vals[i + 2 * stride])
                out[i], out[i + stride], out[i + 2 * stride] = (
                    minus(s2, s1),
                    minus(s0, s2),
                    plus(s2, s1),
                )
        vals = out
    return vals


def combine(terms):
    total = None
    for factor, value in terms:
        if abs(factor) < 1e-12:
            continue
        if abs(factor - 1.0) < 1e-12:
            total = plus(total, value)
        elif abs(factor + 1.0) < 1e-12:
            total = minus(total, value)
        else:
            total = plus(total, value * np.float32(factor))
    return total


def roll(value, shift, axis):
    return value if shift == 0 else pltpu.roll(value, shift % value.shape[axis], axis)


def lane_gather(row, index):
    return jnp.take_along_axis(
        jnp.broadcast_to(row, index.shape), index, axis=1, mode="promise_in_bounds"
    )


def kernel(
    devices_x,
    devices_y,
    gate,
    pop,
    relax,
    solid,
    wall,
    normal,
    count,
    ref,
    stencil,
    weight,
    out,
    vel,
    samples,
    rx_row,
    rx_x,
    post,
    settled,
    shifted,
    fields,
    face,
    near,
    corner,
    got_face,
    got_near,
    got_corner,
    lines,
    masks,
    moved,
    tally,
    send_sem,
    near_sem,
    face_sem,
    far_sem,
    row_ready,
    cross,
    ready,
):
    size_x, size_y = pop.shape[1:3]
    rows = size_x * size_y
    slots_all = wall.shape[2]
    slots = slots_all // devices_y
    shift_bits = slots.bit_length() - 1
    my_x = lax.axis_index("gx")
    my_y = lax.axis_index("gy")
    ratio = np.float32(wall_ratio)
    tile = (size_y, LANES)

    def wrap(value, size):
        return jnp.where(value < 0, value + size, jnp.where(value >= size, value - size, value))

    barrier = pltpu.get_barrier_semaphore()
    columns = {dy: wrap(my_y + dy, devices_y) for dy in range(devices_y)}
    columns[-1] = columns[devices_y - 1]
    beside = {dx: wrap(my_x + dx, devices_x) for dx in (-1, 0, 1)}
    last = devices_x - 1
    inner = my_y - jnp.bitwise_and(my_y, 1)
    outer = inner + 2
    below = jnp.minimum(outer, devices_y)

    def tell(sem, dx, dy):
        pl.semaphore_signal(
            sem,
            inc=1,
            device_id={"gx": beside[dx], "gy": columns[dy]},
            device_id_type=MESH,
        )

    def when(condition, *signal):
        pl.when(condition)(lambda: tell(*signal))

    at_last = my_x == last
    inward = jnp.where(my_x == 0, inner, devices_y)
    outward = jnp.where(at_last, devices_y, inner)
    for dy in range(devices_y):
        when(columns[dy] >= inward, barrier, -1, dy)
    for dy in range(devices_y):
        when(columns[dy] >= outward, barrier, 1, dy)
    for dy in range(1, devices_y):
        when(my_y + dy < devices_y, barrier, 0, dy)

    row_line = lax.broadcasted_iota(jnp.int32, tile, 0)

    moments, speeds = ([], [])
    for x in range(size_x):
        found = forward([pop[i, x] * np.float32(weights[i]) for i in range(27)])
        rho = found[0]
        inverse = 1.0 / rho
        u = [found[9] * inverse, found[3] * inverse, found[1] * inverse]
        for c in range(3):
            vel[c * rows + x * size_y : c * rows + (x + 1) * size_y, :] = u[c]
        moments.append(found)
        speeds.append(u)

    cell = wall[0]
    slot = lax.broadcasted_iota(jnp.int32, (1, slots_all), 1)
    live = slot < count[0, 0]
    which = ref[0]
    row_hit = jnp.logical_and(
        lax.broadcasted_iota(jnp.int32, (rows, slots_all), 0) == jnp.right_shift(cell, 7), live
    )
    values = [
        jnp.right_shift(which, shift_bits) + 1,
        jnp.bitwise_and(which, slots - 1),
        jnp.right_shift(normal[0], 1),
    ]
    left = jnp.concatenate(
        [jnp.where(row_hit, value.astype(jnp.float32), 0.0) for value in values], axis=0
    ).astype(jnp.bfloat16)
    right = jnp.where(
        lax.broadcasted_iota(jnp.int32, (LANES, slots_all), 0)
        == jnp.bitwise_and(cell, LANES - 1),
        1.0,
        0.0,
    ).astype(jnp.bfloat16)
    table = lax.dot_general(
        left, right, (((1,), (1,)), ((), ())), preferred_element_type=jnp.float32
    )

    for part in range(slots_all // LANES):
        lanes = slice(part * LANES, (part + 1) * LANES)
        cells = stencil[0, 0, :, lanes]
        lane = jnp.bitwise_and(cells, LANES - 1)
        row = jnp.right_shift(cells, 7)
        picked = [jnp.zeros(cells.shape, jnp.float32)] * 3
        for r in range(rows):
            here = row == r
            for c in range(3):
                picked[c] = jnp.where(
                    here, lane_gather(vel[c * rows + r : c * rows + r + 1, :], lane), picked[c]
                )
        factor = weight[0, 0, :, lanes]
        for c in range(3):
            n = part * 3 + c
            samples[n : n + 1, :] = jnp.sum(picked[c] * factor, axis=0, keepdims=True)
    rx_row[my_y] = samples[...]

    def equilibrium_terms(n):
        square = [value * value for value in n]
        return 1.0 - 1.5 * (square[0] + square[1] + square[2])

    def along(n, step):
        total = None
        for c in range(3):
            if step[c] > 0:
                total = plus(total, n[c])
            elif step[c] < 0:
                total = minus(total, n[c])
        return total

    def pairs(rho, n):
        rest = rho * equilibrium_terms(n)
        found = {13: rest}
        rho3, rho45 = (rho * 3.0, rho * 4.5)
        for i in range(13):
            s = along(n, steps[i])
            even = rest + rho45 * s * s
            odd = rho3 * s
            found[i], found[26 - i] = (even + odd, even - odd)
        return found

    coefficient = equilibrium_moments()
    rates = [jnp.broadcast_to(relax[0:1, j : j + 1], tile) for j in range(27)]
    near_rows = [
        ((a + 1) * 3 + c + 1, x)
        for a in (-1, 0, 1)
        for c in (-1, 0, 1)
        for x in range(size_x)
        if 0 <= x + a < size_x
    ]
    ends = ((0, size_x - 1), (1, 0))
    for x in range(size_x):
        found, u = (moments[x], speeds[x])
        ux, uy, uz = u
        rho, mx, my, mz = (found[0], found[9], found[3], found[1])
        owner = table[x * size_y : (x + 1) * size_y]
        place = table[rows + x * size_y : rows + (x + 1) * size_y]
        axis = table[2 * rows + x * size_y : 2 * rows + (x + 1) * size_y]
        held = jnp.where(owner > 0.5, rho, 0.0)
        code = jnp.where(owner > 0.5, (owner - 1.0) * np.float32(slots) + place + 1.0, 0.0)
        marked = solid[x].astype(jnp.float32)
        extra = [held, code, axis, marked]
        for f in range(3):
            fields[f, x] = extra[f]
        basis = [rho, mx, my, mz, mx * ux, my * uy, mz * uz, mx * uy, mx * uz, my * uz]
        deviation = []
        for j in range(27):
            if j in (0, 1, 3, 9):
                deviation.append(None)
            else:
                balance = combine(list(zip(coefficient[j], basis)))
                deviation.append(minus(found[j], balance) * rates[j])
        change = backward(deviation)
        local = pairs(held, u)
        for i in range(27):
            a, b, c = steps[i]
            half = 0.5 ** int(np.sum(steps[i] != 0)) / weights[i]
            value = pop[i, x] - change[i] * np.float32(half) - local[i]
            post[i, x] = value
            for way, edge in ends:
                if x == edge and a == 1 - 2 * way:
                    face[way, (b + 1) * 3 + c + 1] = value
            if b != 0:
                side = 0 if b > 0 else 1
                y = size_y - 1 if b > 0 else 0
                line = value[y : y + 1, :]
                j = (a + 1) * 3 + c + 1
                if (j, x) in near_rows:
                    n = near_rows.index((j, x))
                    near[side, n : n + 1, :] = line
                else:
                    corner[0 if a > 0 else 1, side, c + 1 : c + 2, :] = line
        for way, edge in ends:
            if x == edge:
                for f in range(4):
                    face[way, 9 + f] = extra[f]
        for side, y in ((0, size_y - 1), (1, 0)):
            for f in range(4):
                line = extra[f][y : y + 1, :]
                n = len(near_rows) + f * size_x + x
                near[side, n : n + 1, :] = line
                for way, edge in ends:
                    if x == edge:
                        corner[way, side, 3 + f : 4 + f, :] = line

    def send(src, dst, sem, dx, dy):
        pltpu.make_async_remote_copy(
            src_ref=src,
            dst_ref=dst,
            send_sem=send_sem,
            recv_sem=sem,
            device_id={"gx": dx, "gy": columns[dy]},
            device_id_type=MESH,
        ).start()

    across = sorted(range(devices_y), key=lambda dy: -min(dy, devices_y - dy))

    used = 3 * slots_all // LANES

    def send_to(way, dy):
        dx = wrap(my_x + 1 - 2 * way, devices_x)
        send(samples.at[0:used], rx_x.at[way, my_y, 0:used], far_sem.at[way], dx, dy)
        for side, corner_dy in ((0, 1), (1, devices_y - 1)):
            if dy == corner_dy:
                send(corner.at[way, side], got_corner.at[way, side], far_sem.at[way], dx, dy)
        if dy == 0:
            send(face.at[way], got_face.at[way], face_sem.at[way], dx, dy)

    def expect(sem, amount):
        pl.when(amount > 0)(lambda: pl.semaphore_wait(sem, amount))

    def both(first, second):
        return jnp.logical_and(first, second)

    def send_near():
        for side, dy in ((0, 1), (1, -1)):
            send(near.at[side], got_near.at[side], near_sem, my_x, dy)
        for dy in across:
            if dy != 0:
                send(samples.at[0:used], rx_row.at[my_y, 0:used], near_sem, my_x, dy)

    def send_where(way, chosen):
        for dy in across:
            pl.when(chosen[dy])(lambda dy=dy: send_to(way, dy))

    inside = {dy: columns[dy] < outer for dy in across}
    beyond = {dy: columns[dy] >= outer for dy in across}
    beneath = {dy: both(columns[dy] >= inner, columns[dy] < outer) for dy in across}
    top = devices_y - 2
    low = my_y < top
    ahead = [(at_last, 1, 0, 0), (my_x > 0, -1, 1, 2)]
    expect(
        barrier,
        my_y + jnp.where(my_x > 0, below, 0) + jnp.where(at_last, below, 0),
    )
    for applies, dx, way, n in ahead:

        @pl.when(applies)
        def _(dx=dx, way=way, n=n):
            for dy in across:
                when(beneath[dy], ready.at[n], dx, dy)
                when(columns[dy] < inner, ready.at[n + 1], dx, dy)
            send_where(way, inside)

    for dy in range(1, devices_y):
        crossing = both(jnp.logical_not(low), columns[dy] < top) if dy % 2 == 0 else None
        lower = my_y + dy >= devices_y
        if crossing is None:
            when(lower, row_ready, 0, dy)
        else:
            when(crossing, cross, 0, dy)
            when(both(lower, jnp.logical_not(crossing)), row_ready, 0, dy)

    @pl.when(low)
    def _():
        pl.semaphore_wait(cross, 1)
        for applies, dx, way, n in ahead:

            @pl.when(applies)
            def _(way=way):
                send_where(way, beyond)

    expect(row_ready, devices_y - 1 - my_y - jnp.where(low, 1, 0))
    send_near()

    @pl.when(my_x < last)
    def _():
        pl.semaphore_wait(ready.at[2], below - inner)
        send_where(0, inside)
        expect(ready.at[3], devices_y - below)
        send_where(0, beyond)

    def lookup(code, axis, operand, offset):
        r = code.astype(jnp.int32) - 1
        owner = jnp.right_shift(r, shift_bits)
        lane = jnp.bitwise_and(r, slots - 1) + offset
        value = [jnp.zeros(tile, jnp.float32)] * 3
        for peer in range(devices_y):
            here = owner == peer
            for c in range(3):
                value[c] = jnp.where(
                    here,
                    jnp.take_along_axis(operand(peer, c), lane, axis=1, mode="promise_in_bounds"),
                    value[c],
                )
        return [jnp.where(axis == np.float32(c), 0.0, value[c] * ratio) for c in range(3)]

    def spread(line):
        return jnp.broadcast_to(line, tile)

    def part_of(owner):
        return (owner * slots) // LANES * 3, lax.rem(owner * slots, LANES)

    def mend(value, line, b):
        edge = 0 if b > 0 else size_y - 1
        return jnp.where(row_line == edge, spread(line), value)

    part, offset = part_of(my_y)

    near_total = 2 * near.shape[1] + (devices_y - 1) * used
    near_count = pltpu.make_async_copy(
        tally.at[0 : near_total],
        tally.at[0 : near_total],
        near_sem,
    )
    near_count.wait()
    for x in range(size_x):
        n = lookup(
            fields[1, x],
            fields[2, x],
            lambda peer, c: spread(rx_row[peer, pl.ds(part + c, 1), :]),
            offset,
        )
        found = pairs(fields[0, x], n)
        for i in range(27):
            _, b, c = steps[i]
            value = post[i, x] + found[i]
            settled[i, x] = value
            shifted[i, x] = roll(roll(value, b, 0), c, 1)

    for side in range(2):
        for n, (j, x) in enumerate(near_rows):
            q = side * size_x + x
            lines[j, q : q + 1, :] = got_near[side, n : n + 1, :]
        for f in range(4):
            for x in range(size_x):
                n = len(near_rows) + f * size_x + x
                q = side * size_x + x
                lines[9 + f, q : q + 1, :] = got_near[side, n : n + 1, :]
    lower = row_line < size_x
    part0, offset0 = part_of(columns[-1])
    part1, offset1 = part_of(columns[1])
    n = lookup(
        lines[10],
        lines[11],
        lambda peer, c: jnp.where(
            lower,
            spread(rx_row[peer, pl.ds(part0 + c, 1), :]),
            spread(rx_row[peer, pl.ds(part1 + c, 1), :]),
        ),
        jnp.where(lower, offset0, offset1),
    )
    sign_b = jnp.where(lower, 1.0, -1.0)
    n[1] = n[1] * sign_b
    rho = lines[9]
    rest = equilibrium_terms(n)
    border = []
    for j in range(9):
        a, c = (j // 3 - 1, j % 3 - 1)
        s = along(n, (a, 1, c))
        border.append(roll(lines[j] + rho * (rest + s * (3.0 + 4.5 * s)), c, 1))
    marked = [roll(lines[12], c, 1) for c in (-1, 0, 1)]
    for x in range(size_x):
        plane = solid[x].astype(jnp.float32)
        for b in (-1, 0, 1):
            turned = roll(plane, b, 0)
            for c in (-1, 0, 1):
                value = roll(turned, c, 1)
                if b != 0:
                    q = (0 if b > 0 else 1) * size_x + x
                    value = mend(value, marked[c + 1][q : q + 1, :], b)
                masks[(b + 1) * 3 + c + 1, x] = value
    for i in range(27):
        a, b, c = steps[i]
        k = (b + 1) * 3 + c + 1
        for x in range(size_x):
            origin = x - a
            if 0 <= origin < size_x:
                value = shifted[i, origin]
                if b != 0:
                    q = (0 if b > 0 else 1) * size_x + origin
                    value = mend(value, border[(a + 1) * 3 + c + 1][q : q + 1, :], b)
                out[i, x] = jnp.where(masks[k, origin] != 0, settled[26 - i, x], value)

    @pl.when(my_x == 0)
    def _():
        pl.semaphore_wait(ready.at[0], below - inner)
        send_where(1, inside)
        expect(ready.at[1], devices_y - below)
        send_where(1, beyond)

    for way in (1, 0):
        pltpu.make_async_copy(got_face.at[way], got_face.at[way], face_sem.at[way]).wait()
        for k in range(9):
            b, c = (k // 3 - 1, k % 3 - 1)
            moved[way, k] = roll(roll(got_face[way, k], b, 0), c, 1)
            moved[way, 9 + k] = roll(roll(got_face[way, 12], b, 0), c, 1)

    far_total = devices_y * used + 2 * corner.shape[2]
    for way in (1, 0):
        pltpu.make_async_copy(
            tally.at[0:far_total], tally.at[0:far_total], far_sem.at[way]
        ).wait()

    def stack(line):
        return jnp.where(
            row_line == 0,
            spread(line(0, 0)),
            jnp.where(
                row_line == 1,
                spread(line(0, 1)),
                jnp.where(row_line == 2, spread(line(1, 0)), spread(line(1, 1))),
            ),
        )

    quantity = [stack(lambda way, side: got_corner[way, side, f : f + 1, :]) for f in range(7)]
    even = jnp.bitwise_and(row_line, 1) == 0
    parts = (part0, part1)
    n = lookup(
        quantity[4],
        quantity[5],
        lambda peer, c: stack(lambda way, side: rx_x[way, peer, pl.ds(parts[side] + c, 1), :]),
        jnp.where(even, offset0, offset1),
    )
    rest = equilibrium_terms(n)
    s = jnp.where(row_line < 2, n[0], -n[0]) + jnp.where(even, n[1], -n[1])
    corners, marked = ([], [])
    for c in (-1, 0, 1):
        t = s if c == 0 else s + n[2] if c > 0 else s - n[2]
        value = quantity[c + 1] + quantity[3] * (rest + t * (3.0 + 4.5 * t))
        corners.append(roll(value, c, 1))
        marked.append(roll(quantity[6], c, 1))

    for way, a in ((1, -1), (0, 1)):
        n = lookup(
            got_face[way, 10],
            got_face[way, 11],
            lambda peer, c: spread(rx_x[way, peer, pl.ds(part + c, 1), :]),
            offset,
        )
        rho = got_face[way, 9]
        rest = equilibrium_terms(n)
        x = 0 if a > 0 else size_x - 1
        for k in range(9):
            b, c = (k // 3 - 1, k % 3 - 1)
            i = (a + 1) * 9 + k
            s = along(n, (a, b, c))
            value = moved[way, k] + roll(roll(rho * (rest + s * (3.0 + 4.5 * s)), b, 0), c, 1)
            mark = moved[way, 9 + k]
            if b != 0:
                q = way * 2 + (0 if b > 0 else 1)
                value = mend(value, corners[c + 1][q : q + 1, :], b)
                mark = mend(mark, marked[c + 1][q : q + 1, :], b)
            out[i, x] = jnp.where(mark != 0, settled[26 - i, x], value)
    pltpu.make_async_copy(tally, tally, send_sem).wait()


def write_out(source, out, sem):
    copy = pltpu.make_async_copy(source, out, sem)
    copy.start()
    copy.wait()


def pause(out):
    out[...] = jnp.zeros_like(out)


def local(populations, relax, solid, wall_cell, wall_normal, wall_count, sample_ref, cells, factors):
    devices_x, devices_y = (lax.axis_size("gx"), lax.axis_size("gy"))
    size_x, size_y, size_z = populations.shape[1:]
    slots_all = wall_cell.shape[2]
    slots = slots_all // devices_y
    assert size_z == LANES and LANES % slots == 0 and slots & (slots - 1) == 0
    assert slots_all % LANES == 0 and devices_x > 2 and devices_y > 2
    assert devices_y % 2 == 0
    assert 1 < size_x and 2 * size_x <= size_y == 8
    f32 = jnp.float32
    near_lines = -(-(9 * size_x - 6 + 4 * size_x) // 8) * 8
    held = -(-3 * slots_all // LANES // 8) * 8
    used = 3 * slots_all // LANES
    sent = (3 * devices_y - 1) * used + 2 * 13 * size_y + 2 * near_lines + 4 * 8
    vmem = pltpu.VMEM
    tile = (size_y, LANES)
    anywhere = pl.BlockSpec(memory_space=pl.ANY)
    on_core = pl.BlockSpec(memory_space=pltpu.VMEM)
    scalars = pl.BlockSpec(memory_space=pltpu.SMEM)

    def near_core(value):
        return pltpu.with_memory_space_constraint(value, pltpu.VMEM)

    dma = pltpu.SemaphoreType.DMA
    regular = pltpu.SemaphoreType.REGULAR
    gate = pl.pallas_call(
        pause,
        out_shape=pltpu.VMEM(tile, f32),
        out_specs=pl.BlockSpec(memory_space=pltpu.VMEM),
        cost_estimate=pl.CostEstimate(flops=10**9, bytes_accessed=4096, transcendentals=0),
        name="pause",
    )()
    result = pl.pallas_call(
        functools.partial(kernel, devices_x, devices_y),
        out_shape=pltpu.VMEM(populations.shape, f32),
        in_specs=[on_core] * 6 + [scalars] + [on_core] * 3,
        out_specs=pl.BlockSpec(memory_space=pltpu.VMEM),
        scratch_shapes=[
            vmem((3 * size_x * size_y, LANES), f32),
            vmem((held, LANES), f32),
            vmem((devices_y, held, LANES), f32),
            vmem((2, devices_y, held, LANES), f32),
            vmem(populations.shape, f32),
            vmem(populations.shape, f32),
            vmem(populations.shape, f32),
            vmem((3, size_x) + tile, f32),
            vmem((2, 13) + tile, f32),
            vmem((2, near_lines, LANES), f32),
            vmem((2, 2, 8, LANES), f32),
            vmem((2, 13) + tile, f32),
            vmem((2, near_lines, LANES), f32),
            vmem((2, 2, 8, LANES), f32),
            vmem((13,) + tile, f32),
            vmem((9, size_x) + tile, f32),
            vmem((2, 18) + tile, f32),
            vmem((sent, LANES), f32),
            dma,
            dma,
            dma((2,)),
            dma((2,)),
            regular,
            regular,
            regular((4,)),
        ],
        compiler_params=pltpu.CompilerParams(collective_id=0, has_side_effects=True),
        name="lattice_step",
    )(
        pltpu.with_memory_space_constraint(gate, pltpu.VMEM),
        near_core(populations),
        near_core(relax.reshape(1, 27)),
        near_core(solid),
        near_core(wall_cell),
        near_core(wall_normal),
        wall_count,
        near_core(sample_ref),
        near_core(cells),
        near_core(factors),
    )
    result = pltpu.with_memory_space_constraint(result, pltpu.VMEM)
    return pl.pallas_call(
        write_out,
        out_shape=jax.ShapeDtypeStruct(populations.shape, f32),
        in_specs=[pl.BlockSpec(memory_space=pltpu.VMEM)],
        out_specs=anywhere,
        scratch_shapes=[pltpu.SemaphoreType.DMA],
        name="write_out",
    )(result)


def solution(mesh):
    return jax.shard_map(
        local,
        mesh=mesh,
        in_specs=(
            P(None, "gx", "gy", None),
            P(),
            P("gx", "gy", None),
            P("gx", "gy", None),
            P("gx", "gy", None),
            P("gx", "gy"),
            P("gx", "gy", None),
            P("gx", "gy", None, None),
            P("gx", "gy", None, None),
        ),
        out_specs=P(None, "gx", "gy", None),
        check_vma=False,
    )
```

```python
import functools

import jax
import jax.numpy as jnp
import numpy as np
from jax import lax
from jax.experimental import pallas as pl
from jax.experimental.pallas import tpu as pltpu
from jax.sharding import PartitionSpec as P


steps = np.array([(a - 1, b - 1, c - 1) for a in range(3) for b in range(3) for c in range(3)])
wall_ratio = (1.0 / 9.0) ** (1.0 / 7.0)
weights = np.prod(np.where(steps == 0, 2.0 / 3.0, 1.0 / 6.0), axis=1)
vander = np.array([[1.0, 1.0, 1.0], [-1.0, 0.0, 1.0], [1.0, 0.0, 1.0]])
moment = np.kron(np.kron(vander, vander), vander)
LANES = 128
MESH = pl.DeviceIdType.MESH


def equilibrium_moments():
    x, y, z = steps.T.astype(float)
    basis = np.stack(
        [
            np.ones(27),
            3 * x,
            3 * y,
            3 * z,
            4.5 * x * x - 1.5,
            4.5 * y * y - 1.5,
            4.5 * z * z - 1.5,
            9 * x * y,
            9 * x * z,
            9 * y * z,
        ],
        axis=1,
    )
    return moment @ (weights[:, None] * basis)


def forward(vals):
    for stride in (9, 3, 1):
        out = list(vals)
        for i in range(27):
            if i // stride % 3 == 0:
                lo, mid, hi = (vals[i], vals[i + stride], vals[i + 2 * stride])
                both = lo + hi
                out[i], out[i + stride], out[i + 2 * stride] = (both + mid, hi - lo, both)
        vals = out
    return vals


def plus(a, b):
    return b if a is None else a if b is None else a + b


def minus(a, b):
    return a if b is None else -b if a is None else a - b


def backward(vals):
    for stride in (9, 3, 1):
        out = list(vals)
        for i in range(27):
            if i // stride % 3 == 0:
                s0, s1, s2 = (vals[i], vals[i + stride], vals[i + 2 * stride])
                out[i], out[i + stride], out[i + 2 * stride] = (
                    minus(s2, s1),
                    minus(s0, s2),
                    plus(s2, s1),
                )
        vals = out
    return vals


def combine(terms):
    total = None
    for factor, value in terms:
        if abs(factor) < 1e-12:
            continue
        if abs(factor - 1.0) < 1e-12:
            total = plus(total, value)
        elif abs(factor + 1.0) < 1e-12:
            total = minus(total, value)
        else:
            total = plus(total, value * np.float32(factor))
    return total


def roll(value, shift, axis):
    return value if shift == 0 else pltpu.roll(value, shift % value.shape[axis], axis)


def lane_gather(row, index):
    return jnp.take_along_axis(
        jnp.broadcast_to(row, index.shape), index, axis=1, mode="promise_in_bounds"
    )


def kernel(
    devices_x,
    devices_y,
    gate,
    pop,
    relax,
    solid,
    wall,
    normal,
    count,
    ref,
    stencil,
    weight,
    out,
    vel,
    samples,
    rx_row,
    rx_x,
    post,
    settled,
    shifted,
    fields,
    face,
    near,
    corner,
    got_face,
    got_near,
    got_corner,
    lines,
    masks,
    moved,
    tally,
    send_sem,
    near_sem,
    face_sem,
    far_sem,
    row_ready,
    cross,
    ready,
):
    size_x, size_y = pop.shape[1:3]
    rows = size_x * size_y
    slots_all = wall.shape[2]
    slots = slots_all // devices_y
    shift_bits = slots.bit_length() - 1
    my_x = lax.axis_index("gx")
    my_y = lax.axis_index("gy")
    ratio = np.float32(wall_ratio)
    tile = (size_y, LANES)

    def wrap(value, size):
        return jnp.where(value < 0, value + size, jnp.where(value >= size, value - size, value))

    barrier = pltpu.get_barrier_semaphore()
    columns = {dy: wrap(my_y + dy, devices_y) for dy in range(devices_y)}
    columns[-1] = columns[devices_y - 1]
    beside = {dx: wrap(my_x + dx, devices_x) for dx in (-1, 0, 1)}
    last = devices_x - 1
    inner = my_y - jnp.bitwise_and(my_y, 1)
    outer = inner + 2
    below = jnp.minimum(outer, devices_y)

    def tell(sem, dx, dy):
        pl.semaphore_signal(
            sem,
            inc=1,
            device_id={"gx": beside[dx], "gy": columns[dy]},
            device_id_type=MESH,
        )

    def when(condition, *signal):
        pl.when(condition)(lambda: tell(*signal))

    at_last = my_x == last
    inward = jnp.where(my_x == 0, inner, devices_y)
    outward = jnp.where(at_last, devices_y, inner)
    across = sorted(range(devices_y), key=lambda dy: -min(dy, devices_y - dy))
    for dy in across:
        when(columns[dy] >= inward, barrier, -1, dy)
    for dy in across:
        when(columns[dy] >= outward, barrier, 1, dy)
    for dy in range(1, devices_y):
        when(my_y + dy < devices_y, barrier, 0, dy)

    row_line = lax.broadcasted_iota(jnp.int32, tile, 0)

    moments, speeds = ([], [])
    for x in range(size_x):
        found = forward([pop[i, x] * np.float32(weights[i]) for i in range(27)])
        rho = found[0]
        inverse = 1.0 / rho
        u = [found[9] * inverse, found[3] * inverse, found[1] * inverse]
        for c in range(3):
            vel[c * rows + x * size_y : c * rows + (x + 1) * size_y, :] = u[c]
        moments.append(found)
        speeds.append(u)

    cell = wall[0]
    slot = lax.broadcasted_iota(jnp.int32, (1, slots_all), 1)
    live = slot < count[0, 0]
    which = ref[0]
    row_hit = jnp.logical_and(
        lax.broadcasted_iota(jnp.int32, (rows, slots_all), 0) == jnp.right_shift(cell, 7), live
    )
    values = [
        jnp.right_shift(which, shift_bits) + 1,
        jnp.bitwise_and(which, slots - 1),
        jnp.right_shift(normal[0], 1),
    ]
    left = jnp.concatenate(
        [jnp.where(row_hit, value.astype(jnp.float32), 0.0) for value in values], axis=0
    ).astype(jnp.bfloat16)
    right = jnp.where(
        lax.broadcasted_iota(jnp.int32, (LANES, slots_all), 0)
        == jnp.bitwise_and(cell, LANES - 1),
        1.0,
        0.0,
    ).astype(jnp.bfloat16)
    table = lax.dot_general(
        left, right, (((1,), (1,)), ((), ())), preferred_element_type=jnp.float32
    )

    for part in range(slots_all // LANES):
        lanes = slice(part * LANES, (part + 1) * LANES)
        cells = stencil[0, 0, :, lanes]
        lane = jnp.bitwise_and(cells, LANES - 1)
        row = jnp.right_shift(cells, 7)
        picked = [jnp.zeros(cells.shape, jnp.float32)] * 3
        for r in range(rows):
            here = row == r
            for c in range(3):
                picked[c] = jnp.where(
                    here, lane_gather(vel[c * rows + r : c * rows + r + 1, :], lane), picked[c]
                )
        factor = weight[0, 0, :, lanes]
        for c in range(3):
            n = part * 3 + c
            samples[n : n + 1, :] = jnp.sum(picked[c] * factor, axis=0, keepdims=True)
    rx_row[my_y] = samples[...]

    def equilibrium_terms(n):
        square = [value * value for value in n]
        return 1.0 - 1.5 * (square[0] + square[1] + square[2])

    def along(n, step):
        total = None
        for c in range(3):
            if step[c] > 0:
                total = plus(total, n[c])
            elif step[c] < 0:
                total = minus(total, n[c])
        return total

    def pairs(rho, n):
        rest = rho * equilibrium_terms(n)
        found = {13: rest}
        rho3, rho45 = (rho * 3.0, rho * 4.5)
        for i in range(13):
            s = along(n, steps[i])
            even = rest + rho45 * s * s
            odd = rho3 * s
            found[i], found[26 - i] = (even + odd, even - odd)
        return found

    coefficient = equilibrium_moments()
    rates = [jnp.broadcast_to(relax[0:1, j : j + 1], tile) for j in range(27)]
    near_rows = [
        ((a + 1) * 3 + c + 1, x)
        for a in (-1, 0, 1)
        for c in (-1, 0, 1)
        for x in range(size_x)
        if 0 <= x + a < size_x
    ]
    ends = ((0, size_x - 1), (1, 0))
    for x in range(size_x):
        found, u = (moments[x], speeds[x])
        ux, uy, uz = u
        rho, mx, my, mz = (found[0], found[9], found[3], found[1])
        owner = table[x * size_y : (x + 1) * size_y]
        place = table[rows + x * size_y : rows + (x + 1) * size_y]
        axis = table[2 * rows + x * size_y : 2 * rows + (x + 1) * size_y]
        held = jnp.where(owner > 0.5, rho, 0.0)
        code = jnp.where(owner > 0.5, (owner - 1.0) * np.float32(slots) + place + 1.0, 0.0)
        marked = solid[x].astype(jnp.float32)
        extra = [held, code, axis, marked]
        for f in range(3):
            fields[f, x] = extra[f]
        basis = [rho, mx, my, mz, mx * ux, my * uy, mz * uz, mx * uy, mx * uz, my * uz]
        deviation = []
        for j in range(27):
            if j in (0, 1, 3, 9):
                deviation.append(None)
            else:
                balance = combine(list(zip(coefficient[j], basis)))
                deviation.append(minus(found[j], balance) * rates[j])
        change = backward(deviation)
        local = pairs(held, u)
        for i in range(27):
            a, b, c = steps[i]
            half = 0.5 ** int(np.sum(steps[i] != 0)) / weights[i]
            value = pop[i, x] - change[i] * np.float32(half) - local[i]
            post[i, x] = value
            for way, edge in ends:
                if x == edge and a == 1 - 2 * way:
                    face[way, (b + 1) * 3 + c + 1] = value
            if b != 0:
                side = 0 if b > 0 else 1
                y = size_y - 1 if b > 0 else 0
                line = value[y : y + 1, :]
                j = (a + 1) * 3 + c + 1
                if (j, x) in near_rows:
                    n = near_rows.index((j, x))
                    near[side, n : n + 1, :] = line
                else:
                    corner[0 if a > 0 else 1, side, c + 1 : c + 2, :] = line
        for way, edge in ends:
            if x == edge:
                for f in range(4):
                    face[way, 9 + f] = extra[f]
        for side, y in ((0, size_y - 1), (1, 0)):
            for f in range(4):
                line = extra[f][y : y + 1, :]
                n = len(near_rows) + f * size_x + x
                near[side, n : n + 1, :] = line
                for way, edge in ends:
                    if x == edge:
                        corner[way, side, 3 + f : 4 + f, :] = line

    def send(src, dst, sem, dx, dy):
        pltpu.make_async_remote_copy(
            src_ref=src,
            dst_ref=dst,
            send_sem=send_sem,
            recv_sem=sem,
            device_id={"gx": dx, "gy": columns[dy]},
            device_id_type=MESH,
        ).start()


    used = 3 * slots_all // LANES

    def send_to(way, dy):
        dx = wrap(my_x + 1 - 2 * way, devices_x)
        send(samples.at[0:used], rx_x.at[way, my_y, 0:used], far_sem.at[way], dx, dy)
        for side, corner_dy in ((0, 1), (1, devices_y - 1)):
            if dy == corner_dy:
                send(corner.at[way, side], got_corner.at[way, side], far_sem.at[way], dx, dy)
        if dy == 0:
            send(face.at[way], got_face.at[way], face_sem.at[way], dx, dy)

    def expect(sem, amount):
        pl.when(amount > 0)(lambda: pl.semaphore_wait(sem, amount))

    def both(first, second):
        return jnp.logical_and(first, second)

    def send_near():
        for side, dy in ((0, 1), (1, -1)):
            send(near.at[side], got_near.at[side], near_sem, my_x, dy)
        for dy in across:
            if dy != 0:
                send(samples.at[0:used], rx_row.at[my_y, 0:used], near_sem, my_x, dy)

    def send_where(way, chosen):
        for dy in across:
            pl.when(chosen[dy])(lambda dy=dy: send_to(way, dy))

    inside = {dy: columns[dy] < outer for dy in across}
    beyond = {dy: columns[dy] >= outer for dy in across}
    beneath = {dy: both(columns[dy] >= inner, columns[dy] < outer) for dy in across}
    top = devices_y - 2
    low = my_y < top
    ahead = [(at_last, 1, 0, 0), (my_x > 0, -1, 1, 2)]
    expect(
        barrier,
        my_y + jnp.where(my_x > 0, below, 0) + jnp.where(at_last, below, 0),
    )
    for applies, dx, way, n in ahead:

        @pl.when(applies)
        def _(dx=dx, way=way, n=n):
            if way == 0:
                send_where(way, inside)
            for dy in across:
                when(beneath[dy], ready.at[n], dx, dy)
                when(columns[dy] < inner, ready.at[n + 1], dx, dy)
            if way == 1:
                send_where(way, inside)

    for dy in range(1, devices_y):
        crossing = both(jnp.logical_not(low), columns[dy] < top) if dy % 2 == 0 else None
        lower = my_y + dy >= devices_y
        if crossing is None:
            when(lower, row_ready, 0, dy)
        else:
            when(crossing, cross, 0, dy)
            when(both(lower, jnp.logical_not(crossing)), row_ready, 0, dy)

    @pl.when(low)
    def _():
        pl.semaphore_wait(cross, 1)
        for applies, dx, way, n in ahead:

            @pl.when(applies)
            def _(way=way):
                send_where(way, beyond)

    expect(row_ready, devices_y - 1 - my_y - jnp.where(low, 1, 0))
    send_near()

    @pl.when(my_x < last)
    def _():
        pl.semaphore_wait(ready.at[2], below - inner)
        send_where(0, inside)
        expect(ready.at[3], devices_y - below)
        send_where(0, beyond)

    def decode(code, offset):
        r = code.astype(jnp.int32) - 1
        return jnp.right_shift(r, shift_bits), jnp.bitwise_and(r, slots - 1) + offset

    def lookup(owner, lane, axis, operand):
        value = [jnp.zeros(tile, jnp.float32)] * 3
        for peer in range(devices_y):
            here = owner == peer
            for c in range(3):
                value[c] = jnp.where(
                    here,
                    jnp.take_along_axis(operand(peer, c), lane, axis=1, mode="promise_in_bounds"),
                    value[c],
                )
        return [jnp.where(axis == np.float32(c), 0.0, value[c] * ratio) for c in range(3)]

    def spread(line):
        return jnp.broadcast_to(line, tile)

    def part_of(owner):
        return (owner * slots) // LANES * 3, lax.rem(owner * slots, LANES)

    def mend(value, line, b):
        edge = 0 if b > 0 else size_y - 1
        return jnp.where(row_line == edge, spread(line), value)

    part, offset = part_of(my_y)

    near_total = 2 * near.shape[1] + (devices_y - 1) * used
    near_count = pltpu.make_async_copy(
        tally.at[0 : near_total],
        tally.at[0 : near_total],
        near_sem,
    )
    near_count.wait()
    for x in range(size_x):
        n = lookup(
            *decode(fields[1, x], offset),
            fields[2, x],
            lambda peer, c: spread(rx_row[peer, pl.ds(part + c, 1), :]),
        )
        found = pairs(fields[0, x], n)
        for i in range(27):
            _, b, c = steps[i]
            value = post[i, x] + found[i]
            settled[i, x] = value
            shifted[i, x] = roll(roll(value, b, 0), c, 1)

    for side in range(2):
        for n, (j, x) in enumerate(near_rows):
            q = side * size_x + x
            lines[j, q : q + 1, :] = got_near[side, n : n + 1, :]
        for f in range(4):
            for x in range(size_x):
                n = len(near_rows) + f * size_x + x
                q = side * size_x + x
                lines[9 + f, q : q + 1, :] = got_near[side, n : n + 1, :]
    lower = row_line < size_x
    part0, offset0 = part_of(columns[-1])
    part1, offset1 = part_of(columns[1])
    n = lookup(
        *decode(lines[10], jnp.where(lower, offset0, offset1)),
        lines[11],
        lambda peer, c: jnp.where(
            lower,
            spread(rx_row[peer, pl.ds(part0 + c, 1), :]),
            spread(rx_row[peer, pl.ds(part1 + c, 1), :]),
        ),
    )
    sign_b = jnp.where(lower, 1.0, -1.0)
    n[1] = n[1] * sign_b
    rho = lines[9]
    rest = equilibrium_terms(n)
    border = []
    for j in range(9):
        a, c = (j // 3 - 1, j % 3 - 1)
        s = along(n, (a, 1, c))
        border.append(roll(lines[j] + rho * (rest + s * (3.0 + 4.5 * s)), c, 1))
    marked = [roll(lines[12], c, 1) for c in (-1, 0, 1)]
    for x in range(size_x):
        plane = solid[x].astype(jnp.float32)
        for b in (-1, 0, 1):
            turned = roll(plane, b, 0)
            for c in (-1, 0, 1):
                value = roll(turned, c, 1)
                if b != 0:
                    q = (0 if b > 0 else 1) * size_x + x
                    value = mend(value, marked[c + 1][q : q + 1, :], b)
                masks[(b + 1) * 3 + c + 1, x] = value
    for i in range(27):
        a, b, c = steps[i]
        k = (b + 1) * 3 + c + 1
        for x in range(size_x):
            origin = x - a
            if 0 <= origin < size_x:
                value = shifted[i, origin]
                if b != 0:
                    q = (0 if b > 0 else 1) * size_x + origin
                    value = mend(value, border[(a + 1) * 3 + c + 1][q : q + 1, :], b)
                out[i, x] = jnp.where(masks[k, origin] != 0, settled[26 - i, x], value)

    @pl.when(my_x == 0)
    def _():
        pl.semaphore_wait(ready.at[0], below - inner)
        send_where(1, inside)
        expect(ready.at[1], devices_y - below)
        send_where(1, beyond)

    upper = row_line == 0
    sideways = jnp.where(upper, offset0, offset1)

    def stack(one, other):
        return jnp.where(upper, spread(one), spread(other))

    far_total = devices_y * used + 2 * corner.shape[2]
    for way, a in ((1, -1), (0, 1)):
        pltpu.make_async_copy(got_face.at[way], got_face.at[way], face_sem.at[way]).wait()
        for k in range(9):
            b, c = (k // 3 - 1, k % 3 - 1)
            moved[way, k] = roll(roll(got_face[way, k], b, 0), c, 1)
            moved[way, 9 + k] = roll(roll(got_face[way, 12], b, 0), c, 1)
        found_at = decode(got_face[way, 10], offset)
        pltpu.make_async_copy(
            tally.at[0:far_total], tally.at[0:far_total], far_sem.at[way]
        ).wait()
        quantity = [
            stack(got_corner[way, 0, f : f + 1, :], got_corner[way, 1, f : f + 1, :])
            for f in range(7)
        ]
        n = lookup(
            *decode(quantity[4], sideways),
            quantity[5],
            lambda peer, c: stack(
                rx_x[way, peer, pl.ds(part0 + c, 1), :], rx_x[way, peer, pl.ds(part1 + c, 1), :]
            ),
        )
        n[1] = jnp.where(upper, n[1], -n[1])
        rest = equilibrium_terms(n)
        corners, marked = ([], [])
        for c in (-1, 0, 1):
            s = along(n, (a, 1, c))
            value = quantity[c + 1] + quantity[3] * (rest + s * (3.0 + 4.5 * s))
            corners.append(roll(value, c, 1))
            marked.append(roll(quantity[6], c, 1))
        n = lookup(
            *found_at,
            got_face[way, 11],
            lambda peer, c: spread(rx_x[way, peer, pl.ds(part + c, 1), :]),
        )
        rho = got_face[way, 9]
        rest = equilibrium_terms(n)
        x = 0 if a > 0 else size_x - 1
        for k in range(9):
            b, c = (k // 3 - 1, k % 3 - 1)
            i = (a + 1) * 9 + k
            s = along(n, (a, b, c))
            value = moved[way, k] + roll(roll(rho * (rest + s * (3.0 + 4.5 * s)), b, 0), c, 1)
            mark = moved[way, 9 + k]
            if b != 0:
                q = 0 if b > 0 else 1
                value = mend(value, corners[c + 1][q : q + 1, :], b)
                mark = mend(mark, marked[c + 1][q : q + 1, :], b)
            out[i, x] = jnp.where(mark != 0, settled[26 - i, x], value)
    pltpu.make_async_copy(tally, tally, send_sem).wait()


def pause(out):
    out[...] = jnp.zeros_like(out)


def local(populations, relax, solid, wall_cell, wall_normal, wall_count, sample_ref, cells, factors):
    devices_x, devices_y = (lax.axis_size("gx"), lax.axis_size("gy"))
    size_x, size_y, size_z = populations.shape[1:]
    slots_all = wall_cell.shape[2]
    slots = slots_all // devices_y
    assert size_z == LANES and LANES % slots == 0 and slots & (slots - 1) == 0
    assert slots_all % LANES == 0 and devices_x > 2 and devices_y > 2
    assert devices_y % 2 == 0
    assert 1 < size_x and 2 * size_x <= size_y == 8
    f32 = jnp.float32
    near_lines = -(-(9 * size_x - 6 + 4 * size_x) // 8) * 8
    held = -(-3 * slots_all // LANES // 8) * 8
    used = 3 * slots_all // LANES
    sent = (3 * devices_y - 1) * used + 2 * 13 * size_y + 2 * near_lines + 4 * 8
    vmem = pltpu.VMEM
    tile = (size_y, LANES)
    on_core = pl.BlockSpec(memory_space=pltpu.VMEM)
    scalars = pl.BlockSpec(memory_space=pltpu.SMEM)

    def near_core(value):
        return pltpu.with_memory_space_constraint(value, pltpu.VMEM)

    dma = pltpu.SemaphoreType.DMA
    regular = pltpu.SemaphoreType.REGULAR
    gate = pl.pallas_call(
        pause,
        out_shape=pltpu.VMEM(tile, f32),
        out_specs=pl.BlockSpec(memory_space=pltpu.VMEM),
        cost_estimate=pl.CostEstimate(flops=10**9, bytes_accessed=4096, transcendentals=0),
        name="pause",
    )()
    result = pl.pallas_call(
        functools.partial(kernel, devices_x, devices_y),
        out_shape=pltpu.VMEM(populations.shape, f32),
        in_specs=[on_core] * 6 + [scalars] + [on_core] * 3,
        out_specs=pl.BlockSpec(memory_space=pltpu.VMEM),
        scratch_shapes=[
            vmem((3 * size_x * size_y, LANES), f32),
            vmem((held, LANES), f32),
            vmem((devices_y, held, LANES), f32),
            vmem((2, devices_y, held, LANES), f32),
            vmem(populations.shape, f32),
            vmem(populations.shape, f32),
            vmem(populations.shape, f32),
            vmem((3, size_x) + tile, f32),
            vmem((2, 13) + tile, f32),
            vmem((2, near_lines, LANES), f32),
            vmem((2, 2, 8, LANES), f32),
            vmem((2, 13) + tile, f32),
            vmem((2, near_lines, LANES), f32),
            vmem((2, 2, 8, LANES), f32),
            vmem((13,) + tile, f32),
            vmem((9, size_x) + tile, f32),
            vmem((2, 18) + tile, f32),
            vmem((sent, LANES), f32),
            dma,
            dma,
            dma((2,)),
            dma((2,)),
            regular,
            regular,
            regular((4,)),
        ],
        compiler_params=pltpu.CompilerParams(collective_id=0, has_side_effects=True),
        name="lattice_step",
    )(
        pltpu.with_memory_space_constraint(gate, pltpu.VMEM),
        near_core(populations),
        near_core(relax.reshape(1, 27)),
        near_core(solid),
        near_core(wall_cell),
        near_core(wall_normal),
        wall_count,
        near_core(sample_ref),
        near_core(cells),
        near_core(factors),
    )
    return pltpu.with_memory_space_constraint(result, pltpu.VMEM)


def solution(mesh):
    return jax.shard_map(
        local,
        mesh=mesh,
        in_specs=(
            P(None, "gx", "gy", None),
            P(),
            P("gx", "gy", None),
            P("gx", "gy", None),
            P("gx", "gy", None),
            P("gx", "gy"),
            P("gx", "gy", None),
            P("gx", "gy", None, None),
            P("gx", "gy", None, None),
        ),
        out_specs=P(None, "gx", "gy", None),
        check_vma=False,
    )
```

```python
import functools

import jax
import jax.numpy as jnp
import numpy as np
from jax import lax
from jax.experimental import pallas as pl
from jax.experimental.pallas import tpu as pltpu
from jax.sharding import PartitionSpec as P


steps = np.array([(a - 1, b - 1, c - 1) for a in range(3) for b in range(3) for c in range(3)])
wall_ratio = (1.0 / 9.0) ** (1.0 / 7.0)
weights = np.prod(np.where(steps == 0, 2.0 / 3.0, 1.0 / 6.0), axis=1)
vander = np.array([[1.0, 1.0, 1.0], [-1.0, 0.0, 1.0], [1.0, 0.0, 1.0]])
moment = np.kron(np.kron(vander, vander), vander)
LANES = 128
MESH = pl.DeviceIdType.MESH


def equilibrium_moments():
    x, y, z = steps.T.astype(float)
    basis = np.stack(
        [
            np.ones(27),
            3 * x,
            3 * y,
            3 * z,
            4.5 * x * x - 1.5,
            4.5 * y * y - 1.5,
            4.5 * z * z - 1.5,
            9 * x * y,
            9 * x * z,
            9 * y * z,
        ],
        axis=1,
    )
    return moment @ (weights[:, None] * basis)


def forward(vals):
    for stride in (9, 3, 1):
        out = list(vals)
        for i in range(27):
            if i // stride % 3 == 0:
                lo, mid, hi = (vals[i], vals[i + stride], vals[i + 2 * stride])
                both = lo + hi
                out[i], out[i + stride], out[i + 2 * stride] = (both + mid, hi - lo, both)
        vals = out
    return vals


def plus(a, b):
    return b if a is None else a if b is None else a + b


def minus(a, b):
    return a if b is None else -b if a is None else a - b


def backward(vals):
    for stride in (9, 3, 1):
        out = list(vals)
        for i in range(27):
            if i // stride % 3 == 0:
                s0, s1, s2 = (vals[i], vals[i + stride], vals[i + 2 * stride])
                out[i], out[i + stride], out[i + 2 * stride] = (
                    minus(s2, s1),
                    minus(s0, s2),
                    plus(s2, s1),
                )
        vals = out
    return vals


def combine(terms):
    total = None
    for factor, value in terms:
        if abs(factor) < 1e-12:
            continue
        if abs(factor - 1.0) < 1e-12:
            total = plus(total, value)
        elif abs(factor + 1.0) < 1e-12:
            total = minus(total, value)
        else:
            total = plus(total, value * np.float32(factor))
    return total


def roll(value, shift, axis):
    return value if shift == 0 else pltpu.roll(value, shift % value.shape[axis], axis)


def lane_gather(row, index):
    return jnp.take_along_axis(
        jnp.broadcast_to(row, index.shape), index, axis=1, mode="promise_in_bounds"
    )


def equilibrium_terms(n):
    square = [value * value for value in n]
    return 1.0 - 1.5 * (square[0] + square[1] + square[2])


def along(n, step):
    total = None
    for c in range(3):
        if step[c] > 0:
            total = plus(total, n[c])
        elif step[c] < 0:
            total = minus(total, n[c])
    return total


def decode(code, slots, offset):
    r = code.astype(jnp.int32) - 1
    owner = jnp.right_shift(r, slots.bit_length() - 1)
    return owner, jnp.bitwise_and(r, slots - 1) + offset


def lookup(devices_y, owner, lane, axis, operand):
    value = [jnp.zeros(lane.shape, jnp.float32)] * 3
    for peer in range(devices_y):
        here = owner == peer
        for c in range(3):
            value[c] = jnp.where(
                here,
                jnp.take_along_axis(operand(peer, c), lane, axis=1, mode="promise_in_bounds"),
                value[c],
            )
    ratio = np.float32(wall_ratio)
    return [jnp.where(axis == np.float32(c), 0.0, value[c] * ratio) for c in range(3)]


def wrap(value, size):
    return jnp.where(value < 0, value + size, jnp.where(value >= size, value - size, value))


def part_of(owner, slots):
    return (owner * slots) // LANES * 3, lax.rem(owner * slots, LANES)


def mend(value, line, b):
    size_y = value.shape[0]
    row_line = lax.broadcasted_iota(jnp.int32, value.shape, 0)
    edge = 0 if b > 0 else size_y - 1
    return jnp.where(row_line == edge, jnp.broadcast_to(line, value.shape), value)


def far_side(way, devices_y, slots_all, moved, got_face, got_corner, rx_x, settled, x):
    a = 1 - 2 * way
    tile = got_face.shape[2:]
    slots = slots_all // devices_y
    my_y = lax.axis_index("gy")
    part, offset = part_of(my_y, slots)
    part0, offset0 = part_of(wrap(my_y - 1, devices_y), slots)
    part1, offset1 = part_of(wrap(my_y + 1, devices_y), slots)
    upper = lax.broadcasted_iota(jnp.int32, tile, 0) == 0

    def spread(line):
        return jnp.broadcast_to(line, tile)

    def stack(one, other):
        return jnp.where(upper, spread(one), spread(other))

    quantity = [
        stack(got_corner[way, 0, f : f + 1, :], got_corner[way, 1, f : f + 1, :]) for f in range(7)
    ]
    n = lookup(
        devices_y,
        *decode(quantity[4], slots, jnp.where(upper, offset0, offset1)),
        quantity[5],
        lambda peer, c: stack(
            rx_x[way, peer, pl.ds(part0 + c, 1), :], rx_x[way, peer, pl.ds(part1 + c, 1), :]
        ),
    )
    n[1] = jnp.where(upper, n[1], -n[1])
    rest = equilibrium_terms(n)
    corners, marked = ([], [])
    for c in (-1, 0, 1):
        s = along(n, (a, 1, c))
        value = quantity[c + 1] + quantity[3] * (rest + s * (3.0 + 4.5 * s))
        corners.append(roll(value, c, 1))
        marked.append(roll(quantity[6], c, 1))
    n = lookup(
        devices_y,
        *decode(got_face[way, 10], slots, offset),
        got_face[way, 11],
        lambda peer, c: spread(rx_x[way, peer, pl.ds(part + c, 1), :]),
    )
    rho = got_face[way, 9]
    rest = equilibrium_terms(n)
    tiles = []
    for k in range(9):
        b, c = (k // 3 - 1, k % 3 - 1)
        i = (a + 1) * 9 + k
        s = along(n, (a, b, c))
        value = moved[way, k] + roll(roll(rho * (rest + s * (3.0 + 4.5 * s)), b, 0), c, 1)
        mark = moved[way, 9 + k]
        if b != 0:
            q = 0 if b > 0 else 1
            value = mend(value, corners[c + 1][q : q + 1, :], b)
            mark = mend(mark, marked[c + 1][q : q + 1, :], b)
        tiles.append(jnp.where(mark != 0, settled[26 - i, x], value))
    return tiles


def finish(devices_y, slots_all, early, settled, moved, got_face, got_corner, rx_x, out, late, sem):
    copies = [
        pltpu.make_async_copy(early.at[0:18], out.at[0:18], sem.at[0]),
        pltpu.make_async_copy(early.at[18:27, 1:], out.at[18:27, 1:], sem.at[1]),
        pltpu.make_async_copy(late, out.at[18:27, 0], sem.at[2]),
    ]
    copies[0].start()
    copies[1].start()
    tiles = far_side(0, devices_y, slots_all, moved, got_face, got_corner, rx_x, settled, 0)
    for k, value in enumerate(tiles):
        late[k] = value
    copies[2].start()
    for copy in copies:
        copy.wait()


def kernel(
    devices_x,
    devices_y,
    gate,
    pop,
    relax,
    solid,
    wall,
    normal,
    count,
    ref,
    stencil,
    weight,
    out,
    settled,
    moved,
    got_face,
    got_corner,
    rx_x,
    vel,
    samples,
    rx_row,
    post,
    shifted,
    fields,
    face,
    near,
    corner,
    got_near,
    lines,
    masks,
    tally,
    send_sem,
    near_sem,
    face_sem,
    far_sem,
    row_ready,
    cross,
    ready,
):
    size_x, size_y = pop.shape[1:3]
    rows = size_x * size_y
    slots_all = wall.shape[2]
    slots = slots_all // devices_y
    shift_bits = slots.bit_length() - 1
    my_x = lax.axis_index("gx")
    my_y = lax.axis_index("gy")
    tile = (size_y, LANES)

    barrier = pltpu.get_barrier_semaphore()
    columns = {dy: wrap(my_y + dy, devices_y) for dy in range(devices_y)}
    columns[-1] = columns[devices_y - 1]
    beside = {dx: wrap(my_x + dx, devices_x) for dx in (-1, 0, 1)}
    last = devices_x - 1
    inner = my_y - jnp.bitwise_and(my_y, 1)
    outer = inner + 2
    below = jnp.minimum(outer, devices_y)

    def tell(sem, dx, dy):
        pl.semaphore_signal(
            sem,
            inc=1,
            device_id={"gx": beside[dx], "gy": columns[dy]},
            device_id_type=MESH,
        )

    def when(condition, *signal):
        pl.when(condition)(lambda: tell(*signal))

    at_last = my_x == last
    inward = jnp.where(my_x == 0, inner, devices_y)
    outward = jnp.where(at_last, devices_y, inner)
    across = sorted(range(devices_y), key=lambda dy: -min(dy, devices_y - dy))
    for dy in across:
        when(columns[dy] >= inward, barrier, -1, dy)
    for dy in across:
        when(columns[dy] >= outward, barrier, 1, dy)
    for dy in range(1, devices_y):
        when(my_y + dy < devices_y, barrier, 0, dy)

    row_line = lax.broadcasted_iota(jnp.int32, tile, 0)

    moments, speeds = ([], [])
    for x in range(size_x):
        found = forward([pop[i, x] * np.float32(weights[i]) for i in range(27)])
        rho = found[0]
        inverse = 1.0 / rho
        u = [found[9] * inverse, found[3] * inverse, found[1] * inverse]
        for c in range(3):
            vel[c * rows + x * size_y : c * rows + (x + 1) * size_y, :] = u[c]
        moments.append(found)
        speeds.append(u)

    cell = wall[0]
    slot = lax.broadcasted_iota(jnp.int32, (1, slots_all), 1)
    live = slot < count[0, 0]
    which = ref[0]
    row_hit = jnp.logical_and(
        lax.broadcasted_iota(jnp.int32, (rows, slots_all), 0) == jnp.right_shift(cell, 7), live
    )
    values = [
        jnp.right_shift(which, shift_bits) + 1,
        jnp.bitwise_and(which, slots - 1),
        jnp.right_shift(normal[0], 1),
    ]
    left = jnp.concatenate(
        [jnp.where(row_hit, value.astype(jnp.float32), 0.0) for value in values], axis=0
    ).astype(jnp.bfloat16)
    right = jnp.where(
        lax.broadcasted_iota(jnp.int32, (LANES, slots_all), 0)
        == jnp.bitwise_and(cell, LANES - 1),
        1.0,
        0.0,
    ).astype(jnp.bfloat16)
    table = lax.dot_general(
        left, right, (((1,), (1,)), ((), ())), preferred_element_type=jnp.float32
    )

    for part in range(slots_all // LANES):
        lanes = slice(part * LANES, (part + 1) * LANES)
        cells = stencil[0, 0, :, lanes]
        lane = jnp.bitwise_and(cells, LANES - 1)
        row = jnp.right_shift(cells, 7)
        picked = [jnp.zeros(cells.shape, jnp.float32)] * 3
        for r in range(rows):
            here = row == r
            for c in range(3):
                picked[c] = jnp.where(
                    here, lane_gather(vel[c * rows + r : c * rows + r + 1, :], lane), picked[c]
                )
        factor = weight[0, 0, :, lanes]
        for c in range(3):
            n = part * 3 + c
            samples[n : n + 1, :] = jnp.sum(picked[c] * factor, axis=0, keepdims=True)
    rx_row[my_y] = samples[...]

    def pairs(rho, n):
        rest = rho * equilibrium_terms(n)
        found = {13: rest}
        rho3, rho45 = (rho * 3.0, rho * 4.5)
        for i in range(13):
            s = along(n, steps[i])
            even = rest + rho45 * s * s
            odd = rho3 * s
            found[i], found[26 - i] = (even + odd, even - odd)
        return found

    coefficient = equilibrium_moments()
    rates = [jnp.broadcast_to(relax[0:1, j : j + 1], tile) for j in range(27)]
    near_rows = [
        ((a + 1) * 3 + c + 1, x)
        for a in (-1, 0, 1)
        for c in (-1, 0, 1)
        for x in range(size_x)
        if 0 <= x + a < size_x
    ]
    ends = ((0, size_x - 1), (1, 0))
    for x in range(size_x):
        found, u = (moments[x], speeds[x])
        ux, uy, uz = u
        rho, mx, my, mz = (found[0], found[9], found[3], found[1])
        owner = table[x * size_y : (x + 1) * size_y]
        place = table[rows + x * size_y : rows + (x + 1) * size_y]
        axis = table[2 * rows + x * size_y : 2 * rows + (x + 1) * size_y]
        held = jnp.where(owner > 0.5, rho, 0.0)
        code = jnp.where(owner > 0.5, (owner - 1.0) * np.float32(slots) + place + 1.0, 0.0)
        marked = solid[x].astype(jnp.float32)
        extra = [held, code, axis, marked]
        for f in range(3):
            fields[f, x] = extra[f]
        basis = [rho, mx, my, mz, mx * ux, my * uy, mz * uz, mx * uy, mx * uz, my * uz]
        deviation = []
        for j in range(27):
            if j in (0, 1, 3, 9):
                deviation.append(None)
            else:
                balance = combine(list(zip(coefficient[j], basis)))
                deviation.append(minus(found[j], balance) * rates[j])
        change = backward(deviation)
        local = pairs(held, u)
        for i in range(27):
            a, b, c = steps[i]
            half = 0.5 ** int(np.sum(steps[i] != 0)) / weights[i]
            value = pop[i, x] - change[i] * np.float32(half) - local[i]
            post[i, x] = value
            for way, edge in ends:
                if x == edge and a == 1 - 2 * way:
                    face[way, (b + 1) * 3 + c + 1] = value
            if b != 0:
                side = 0 if b > 0 else 1
                y = size_y - 1 if b > 0 else 0
                line = value[y : y + 1, :]
                j = (a + 1) * 3 + c + 1
                if (j, x) in near_rows:
                    n = near_rows.index((j, x))
                    near[side, n : n + 1, :] = line
                else:
                    corner[0 if a > 0 else 1, side, c + 1 : c + 2, :] = line
        for way, edge in ends:
            if x == edge:
                for f in range(4):
                    face[way, 9 + f] = extra[f]
        for side, y in ((0, size_y - 1), (1, 0)):
            for f in range(4):
                line = extra[f][y : y + 1, :]
                n = len(near_rows) + f * size_x + x
                near[side, n : n + 1, :] = line
                for way, edge in ends:
                    if x == edge:
                        corner[way, side, 3 + f : 4 + f, :] = line

    def send(src, dst, sem, dx, dy):
        pltpu.make_async_remote_copy(
            src_ref=src,
            dst_ref=dst,
            send_sem=send_sem,
            recv_sem=sem,
            device_id={"gx": dx, "gy": columns[dy]},
            device_id_type=MESH,
        ).start()


    used = 3 * slots_all // LANES

    def send_to(way, dy):
        dx = wrap(my_x + 1 - 2 * way, devices_x)
        send(samples.at[0:used], rx_x.at[way, my_y, 0:used], far_sem.at[way], dx, dy)
        for side, corner_dy in ((0, 1), (1, devices_y - 1)):
            if dy == corner_dy:
                send(corner.at[way, side], got_corner.at[way, side], far_sem.at[way], dx, dy)
        if dy == 0:
            send(face.at[way], got_face.at[way], face_sem.at[way], dx, dy)

    def expect(sem, amount):
        pl.when(amount > 0)(lambda: pl.semaphore_wait(sem, amount))

    def both(first, second):
        return jnp.logical_and(first, second)

    def send_near():
        for side, dy in ((0, 1), (1, -1)):
            send(near.at[side], got_near.at[side], near_sem, my_x, dy)
        for dy in across:
            if dy != 0:
                send(samples.at[0:used], rx_row.at[my_y, 0:used], near_sem, my_x, dy)

    def send_where(way, chosen):
        for dy in across:
            pl.when(chosen[dy])(lambda dy=dy: send_to(way, dy))

    inside = {dy: columns[dy] < outer for dy in across}
    beyond = {dy: columns[dy] >= outer for dy in across}
    beneath = {dy: both(columns[dy] >= inner, columns[dy] < outer) for dy in across}
    top = devices_y - 2
    low = my_y < top
    ahead = [(at_last, 1, 0, 0), (my_x > 0, -1, 1, 2)]
    expect(
        barrier,
        my_y + jnp.where(my_x > 0, below, 0) + jnp.where(at_last, below, 0),
    )
    for applies, dx, way, n in ahead:

        @pl.when(applies)
        def _(dx=dx, way=way, n=n):
            if way == 0:
                send_where(way, inside)
            for dy in across:
                when(beneath[dy], ready.at[n], dx, dy)
                when(columns[dy] < inner, ready.at[n + 1], dx, dy)
            if way == 1:
                send_where(way, inside)

    for dy in range(1, devices_y):
        crossing = both(jnp.logical_not(low), columns[dy] < top) if dy % 2 == 0 else None
        lower = my_y + dy >= devices_y
        if crossing is None:
            when(lower, row_ready, 0, dy)
        else:
            when(crossing, cross, 0, dy)
            when(both(lower, jnp.logical_not(crossing)), row_ready, 0, dy)

    @pl.when(low)
    def _():
        pl.semaphore_wait(cross, 1)
        for applies, dx, way, n in ahead:

            @pl.when(applies)
            def _(way=way):
                send_where(way, beyond)

    expect(row_ready, devices_y - 1 - my_y - jnp.where(low, 1, 0))
    send_near()

    @pl.when(my_x < last)
    def _():
        pl.semaphore_wait(ready.at[2], below - inner)
        send_where(0, inside)
        expect(ready.at[3], devices_y - below)
        send_where(0, beyond)

    def spread(line):
        return jnp.broadcast_to(line, tile)

    part, offset = part_of(my_y, slots)

    near_total = 2 * near.shape[1] + (devices_y - 1) * used
    near_count = pltpu.make_async_copy(
        tally.at[0 : near_total],
        tally.at[0 : near_total],
        near_sem,
    )
    near_count.wait()
    for x in range(size_x):
        n = lookup(
            devices_y,
            *decode(fields[1, x], slots, offset),
            fields[2, x],
            lambda peer, c: spread(rx_row[peer, pl.ds(part + c, 1), :]),
        )
        found = pairs(fields[0, x], n)
        for i in range(27):
            _, b, c = steps[i]
            value = post[i, x] + found[i]
            settled[i, x] = value
            shifted[i, x] = roll(roll(value, b, 0), c, 1)

    for side in range(2):
        for n, (j, x) in enumerate(near_rows):
            q = side * size_x + x
            lines[j, q : q + 1, :] = got_near[side, n : n + 1, :]
        for f in range(4):
            for x in range(size_x):
                n = len(near_rows) + f * size_x + x
                q = side * size_x + x
                lines[9 + f, q : q + 1, :] = got_near[side, n : n + 1, :]
    lower = row_line < size_x
    part0, offset0 = part_of(columns[-1], slots)
    part1, offset1 = part_of(columns[1], slots)
    n = lookup(
        devices_y,
        *decode(lines[10], slots, jnp.where(lower, offset0, offset1)),
        lines[11],
        lambda peer, c: jnp.where(
            lower,
            spread(rx_row[peer, pl.ds(part0 + c, 1), :]),
            spread(rx_row[peer, pl.ds(part1 + c, 1), :]),
        ),
    )
    sign_b = jnp.where(lower, 1.0, -1.0)
    n[1] = n[1] * sign_b
    rho = lines[9]
    rest = equilibrium_terms(n)
    border = []
    for j in range(9):
        a, c = (j // 3 - 1, j % 3 - 1)
        s = along(n, (a, 1, c))
        border.append(roll(lines[j] + rho * (rest + s * (3.0 + 4.5 * s)), c, 1))
    marked = [roll(lines[12], c, 1) for c in (-1, 0, 1)]
    for x in range(size_x):
        plane = solid[x].astype(jnp.float32)
        for b in (-1, 0, 1):
            turned = roll(plane, b, 0)
            for c in (-1, 0, 1):
                value = roll(turned, c, 1)
                if b != 0:
                    q = (0 if b > 0 else 1) * size_x + x
                    value = mend(value, marked[c + 1][q : q + 1, :], b)
                masks[(b + 1) * 3 + c + 1, x] = value
    for i in range(27):
        a, b, c = steps[i]
        k = (b + 1) * 3 + c + 1
        for x in range(size_x):
            origin = x - a
            if 0 <= origin < size_x:
                value = shifted[i, origin]
                if b != 0:
                    q = (0 if b > 0 else 1) * size_x + origin
                    value = mend(value, border[(a + 1) * 3 + c + 1][q : q + 1, :], b)
                out[i, x] = jnp.where(masks[k, origin] != 0, settled[26 - i, x], value)

    @pl.when(my_x == 0)
    def _():
        pl.semaphore_wait(ready.at[0], below - inner)
        send_where(1, inside)
        expect(ready.at[1], devices_y - below)
        send_where(1, beyond)

    far_total = devices_y * used + 2 * corner.shape[2]
    for way, a in ((1, -1), (0, 1)):
        pltpu.make_async_copy(got_face.at[way], got_face.at[way], face_sem.at[way]).wait()
        for k in range(9):
            b, c = (k // 3 - 1, k % 3 - 1)
            moved[way, k] = roll(roll(got_face[way, k], b, 0), c, 1)
            moved[way, 9 + k] = roll(roll(got_face[way, 12], b, 0), c, 1)
        pltpu.make_async_copy(
            tally.at[0:far_total], tally.at[0:far_total], far_sem.at[way]
        ).wait()
        if way == 1:
            x = size_x - 1
            tiles = far_side(
                way, devices_y, slots_all, moved, got_face, got_corner, rx_x, settled, x
            )
            for k, value in enumerate(tiles):
                out[k, x] = value
    pltpu.make_async_copy(tally, tally, send_sem).wait()


def pause(out):
    out[...] = jnp.zeros_like(out)


def local(populations, relax, solid, wall_cell, wall_normal, wall_count, sample_ref, cells, factors):
    devices_x, devices_y = (lax.axis_size("gx"), lax.axis_size("gy"))
    size_x, size_y, size_z = populations.shape[1:]
    slots_all = wall_cell.shape[2]
    slots = slots_all // devices_y
    assert size_z == LANES and LANES % slots == 0 and slots & (slots - 1) == 0
    assert slots_all % LANES == 0 and devices_x > 2 and devices_y > 2
    assert devices_y % 2 == 0
    assert 1 < size_x and 2 * size_x <= size_y == 8
    f32 = jnp.float32
    near_lines = -(-(9 * size_x - 6 + 4 * size_x) // 8) * 8
    held = -(-3 * slots_all // LANES // 8) * 8
    used = 3 * slots_all // LANES
    sent = (3 * devices_y - 1) * used + 2 * 13 * size_y + 2 * near_lines + 4 * 8
    vmem = pltpu.VMEM
    tile = (size_y, LANES)
    on_core = pl.BlockSpec(memory_space=pltpu.VMEM)
    scalars = pl.BlockSpec(memory_space=pltpu.SMEM)

    def near_core(value):
        return pltpu.with_memory_space_constraint(value, pltpu.VMEM)

    dma = pltpu.SemaphoreType.DMA
    regular = pltpu.SemaphoreType.REGULAR
    gate = pl.pallas_call(
        pause,
        out_shape=pltpu.VMEM(tile, f32),
        out_specs=pl.BlockSpec(memory_space=pltpu.VMEM),
        cost_estimate=pl.CostEstimate(flops=10**9, bytes_accessed=4096, transcendentals=0),
        name="pause",
    )()
    kept = [
        populations.shape,
        populations.shape,
        (2, 18) + tile,
        (2, 13) + tile,
        (2, 2, 8, LANES),
        (2, devices_y, held, LANES),
    ]
    results = pl.pallas_call(
        functools.partial(kernel, devices_x, devices_y),
        out_shape=[pltpu.VMEM(shape, f32) for shape in kept],
        in_specs=[on_core] * 6 + [scalars] + [on_core] * 3,
        out_specs=[on_core] * len(kept),
        scratch_shapes=[
            vmem((3 * size_x * size_y, LANES), f32),
            vmem((held, LANES), f32),
            vmem((devices_y, held, LANES), f32),
            vmem(populations.shape, f32),
            vmem(populations.shape, f32),
            vmem((3, size_x) + tile, f32),
            vmem((2, 13) + tile, f32),
            vmem((2, near_lines, LANES), f32),
            vmem((2, 2, 8, LANES), f32),
            vmem((2, near_lines, LANES), f32),
            vmem((13,) + tile, f32),
            vmem((9, size_x) + tile, f32),
            vmem((sent, LANES), f32),
            dma,
            dma,
            dma((2,)),
            dma((2,)),
            regular,
            regular,
            regular((4,)),
        ],
        compiler_params=pltpu.CompilerParams(collective_id=0, has_side_effects=True),
        name="lattice_step",
    )(
        pltpu.with_memory_space_constraint(gate, pltpu.VMEM),
        near_core(populations),
        near_core(relax.reshape(1, 27)),
        near_core(solid),
        near_core(wall_cell),
        near_core(wall_normal),
        wall_count,
        near_core(sample_ref),
        near_core(cells),
        near_core(factors),
    )
    return pl.pallas_call(
        functools.partial(finish, devices_y, slots_all),
        out_shape=jax.ShapeDtypeStruct(populations.shape, f32),
        in_specs=[on_core] * len(kept),
        out_specs=pl.BlockSpec(memory_space=pl.ANY),
        scratch_shapes=[vmem((9,) + tile, f32), dma((3,))],
        name="finish",
    )(*[near_core(value) for value in results])


def solution(mesh):
    return jax.shard_map(
        local,
        mesh=mesh,
        in_specs=(
            P(None, "gx", "gy", None),
            P(),
            P("gx", "gy", None),
            P("gx", "gy", None),
            P("gx", "gy", None),
            P("gx", "gy"),
            P("gx", "gy", None),
            P("gx", "gy", None, None),
            P("gx", "gy", None, None),
        ),
        out_specs=P(None, "gx", "gy", None),
        check_vma=False,
    )
```

```python
import functools

import jax
import jax.numpy as jnp
import numpy as np
from jax import lax
from jax.experimental import pallas as pl
from jax.experimental.pallas import tpu as pltpu
from jax.sharding import PartitionSpec as P


steps = np.array([(a - 1, b - 1, c - 1) for a in range(3) for b in range(3) for c in range(3)])
wall_ratio = (1.0 / 9.0) ** (1.0 / 7.0)
weights = np.prod(np.where(steps == 0, 2.0 / 3.0, 1.0 / 6.0), axis=1)
vander = np.array([[1.0, 1.0, 1.0], [-1.0, 0.0, 1.0], [1.0, 0.0, 1.0]])
moment = np.kron(np.kron(vander, vander), vander)
LANES = 128
MESH = pl.DeviceIdType.MESH


def equilibrium_moments():
    x, y, z = steps.T.astype(float)
    basis = np.stack(
        [
            np.ones(27),
            3 * x,
            3 * y,
            3 * z,
            4.5 * x * x - 1.5,
            4.5 * y * y - 1.5,
            4.5 * z * z - 1.5,
            9 * x * y,
            9 * x * z,
            9 * y * z,
        ],
        axis=1,
    )
    return moment @ (weights[:, None] * basis)


def forward(vals):
    for stride in (9, 3, 1):
        out = list(vals)
        for i in range(27):
            if i // stride % 3 == 0:
                lo, mid, hi = (vals[i], vals[i + stride], vals[i + 2 * stride])
                both = lo + hi
                out[i], out[i + stride], out[i + 2 * stride] = (both + mid, hi - lo, both)
        vals = out
    return vals


def plus(a, b):
    return b if a is None else a if b is None else a + b


def minus(a, b):
    return a if b is None else -b if a is None else a - b


def backward(vals):
    for stride in (9, 3, 1):
        out = list(vals)
        for i in range(27):
            if i // stride % 3 == 0:
                s0, s1, s2 = (vals[i], vals[i + stride], vals[i + 2 * stride])
                out[i], out[i + stride], out[i + 2 * stride] = (
                    minus(s2, s1),
                    minus(s0, s2),
                    plus(s2, s1),
                )
        vals = out
    return vals


def combine(terms):
    total = None
    for factor, value in terms:
        if abs(factor) < 1e-12:
            continue
        if abs(factor - 1.0) < 1e-12:
            total = plus(total, value)
        elif abs(factor + 1.0) < 1e-12:
            total = minus(total, value)
        else:
            total = plus(total, value * np.float32(factor))
    return total


def roll(value, shift, axis):
    return value if shift == 0 else pltpu.roll(value, shift % value.shape[axis], axis)


def lane_gather(row, index):
    return jnp.take_along_axis(
        jnp.broadcast_to(row, index.shape), index, axis=1, mode="promise_in_bounds"
    )


def equilibrium_terms(n):
    square = [value * value for value in n]
    return 1.0 - 1.5 * (square[0] + square[1] + square[2])


def along(n, step):
    total = None
    for c in range(3):
        if step[c] > 0:
            total = plus(total, n[c])
        elif step[c] < 0:
            total = minus(total, n[c])
    return total


def decode(code, slots, offset):
    r = code.astype(jnp.int32) - 1
    owner = jnp.right_shift(r, slots.bit_length() - 1)
    return owner, jnp.bitwise_and(r, slots - 1) + offset


def lookup(devices_y, owner, lane, axis, operand):
    value = [jnp.zeros(lane.shape, jnp.float32)] * 3
    for peer in range(devices_y):
        here = owner == peer
        for c in range(3):
            value[c] = jnp.where(
                here,
                jnp.take_along_axis(operand(peer, c), lane, axis=1, mode="promise_in_bounds"),
                value[c],
            )
    ratio = np.float32(wall_ratio)
    return [jnp.where(axis == np.float32(c), 0.0, value[c] * ratio) for c in range(3)]


def wrap(value, size):
    return jnp.where(value < 0, value + size, jnp.where(value >= size, value - size, value))


def part_of(owner, slots):
    return (owner * slots) // LANES * 3, lax.rem(owner * slots, LANES)


def mend(value, line, b):
    size_y = value.shape[0]
    row_line = lax.broadcasted_iota(jnp.int32, value.shape, 0)
    edge = 0 if b > 0 else size_y - 1
    return jnp.where(row_line == edge, jnp.broadcast_to(line, value.shape), value)


def far_side(way, devices_y, slots_all, moved, got_face, got_corner, rx_x, settled, x):
    a = 1 - 2 * way
    tile = got_face.shape[2:]
    slots = slots_all // devices_y
    my_y = lax.axis_index("gy")
    part, offset = part_of(my_y, slots)
    part0, offset0 = part_of(wrap(my_y - 1, devices_y), slots)
    part1, offset1 = part_of(wrap(my_y + 1, devices_y), slots)
    upper = lax.broadcasted_iota(jnp.int32, tile, 0) == 0

    def spread(line):
        return jnp.broadcast_to(line, tile)

    def stack(one, other):
        return jnp.where(upper, spread(one), spread(other))

    quantity = [
        stack(got_corner[way, 0, f : f + 1, :], got_corner[way, 1, f : f + 1, :]) for f in range(7)
    ]
    n = lookup(
        devices_y,
        *decode(quantity[4], slots, jnp.where(upper, offset0, offset1)),
        quantity[5],
        lambda peer, c: stack(
            rx_x[way, peer, pl.ds(part0 + c, 1), :], rx_x[way, peer, pl.ds(part1 + c, 1), :]
        ),
    )
    n[1] = jnp.where(upper, n[1], -n[1])
    rest = equilibrium_terms(n)
    corners, marked = ([], [])
    for c in (-1, 0, 1):
        s = along(n, (a, 1, c))
        value = quantity[c + 1] + quantity[3] * (rest + s * (3.0 + 4.5 * s))
        corners.append(roll(value, c, 1))
        marked.append(roll(quantity[6], c, 1))
    n = lookup(
        devices_y,
        *decode(got_face[way, 10], slots, offset),
        got_face[way, 11],
        lambda peer, c: spread(rx_x[way, peer, pl.ds(part + c, 1), :]),
    )
    rho = got_face[way, 9]
    rest = equilibrium_terms(n)
    tiles = []
    for k in range(9):
        b, c = (k // 3 - 1, k % 3 - 1)
        i = (a + 1) * 9 + k
        s = along(n, (a, b, c))
        value = moved[way, k] + roll(roll(rho * (rest + s * (3.0 + 4.5 * s)), b, 0), c, 1)
        mark = moved[way, 9 + k]
        if b != 0:
            q = 0 if b > 0 else 1
            value = mend(value, corners[c + 1][q : q + 1, :], b)
            mark = mend(mark, marked[c + 1][q : q + 1, :], b)
        tiles.append(jnp.where(mark != 0, settled[26 - i, x], value))
    return tiles


def finish(devices_y, slots_all, early, settled, moved, got_face, got_corner, rx_x, out, late, sem):
    copies = [
        pltpu.make_async_copy(early.at[0:18], out.at[0:18], sem.at[0]),
        pltpu.make_async_copy(early.at[18:27, 1:], out.at[18:27, 1:], sem.at[1]),
        pltpu.make_async_copy(late, out.at[18:27, 0], sem.at[2]),
    ]
    copies[0].start()
    copies[1].start()
    tiles = far_side(0, devices_y, slots_all, moved, got_face, got_corner, rx_x, settled, 0)
    for k, value in enumerate(tiles):
        late[k] = value
    copies[2].start()
    for copy in copies:
        copy.wait()


def kernel(
    devices_x,
    devices_y,
    gate,
    pop,
    relax,
    solid,
    wall,
    normal,
    count,
    ref,
    stencil,
    weight,
    out,
    settled,
    moved,
    got_face,
    got_corner,
    rx_x,
    vel,
    samples,
    rx_row,
    post,
    shifted,
    fields,
    face,
    near,
    corner,
    got_near,
    lines,
    masks,
    tally,
    send_sem,
    near_sem,
    face_sem,
    far_sem,
    row_ready,
    cross,
    ready,
):
    size_x, size_y = pop.shape[1:3]
    rows = size_x * size_y
    slots_all = wall.shape[2]
    slots = slots_all // devices_y
    shift_bits = slots.bit_length() - 1
    my_x = lax.axis_index("gx")
    my_y = lax.axis_index("gy")
    tile = (size_y, LANES)

    barrier = pltpu.get_barrier_semaphore()
    columns = {dy: wrap(my_y + dy, devices_y) for dy in range(devices_y)}
    columns[-1] = columns[devices_y - 1]
    beside = {dx: wrap(my_x + dx, devices_x) for dx in (-1, 0, 1)}
    last = devices_x - 1
    inner = my_y - jnp.bitwise_and(my_y, 1)
    outer = inner + 2
    below = jnp.minimum(outer, devices_y)

    def tell(sem, dx, dy):
        pl.semaphore_signal(
            sem,
            inc=1,
            device_id={"gx": beside[dx], "gy": columns[dy]},
            device_id_type=MESH,
        )

    def when(condition, *signal):
        pl.when(condition)(lambda: tell(*signal))

    at_last = my_x == last
    inward = jnp.where(my_x == 0, inner, devices_y)
    outward = jnp.where(at_last, devices_y, inner)
    across = sorted(range(devices_y), key=lambda dy: -min(dy, devices_y - dy))
    for dy in across:

        @pl.when(columns[dy] >= inward)
        def _(dy=dy):
            pl.semaphore_signal(
                barrier,
                inc=1,
                device_id={"gx": last, "gy": columns[dy]},
                device_id_type=MESH,
            )

    for dy in across:
        when(columns[dy] >= outward, barrier, 1, dy)
    for dy in range(1, devices_y):
        when(my_y + dy < devices_y, barrier, 0, dy)

    row_line = lax.broadcasted_iota(jnp.int32, tile, 0)

    moments, speeds = ([], [])
    for x in range(size_x):
        found = forward([pop[i, x] * np.float32(weights[i]) for i in range(27)])
        rho = found[0]
        inverse = 1.0 / rho
        u = [found[9] * inverse, found[3] * inverse, found[1] * inverse]
        for c in range(3):
            vel[c * rows + x * size_y : c * rows + (x + 1) * size_y, :] = u[c]
        moments.append(found)
        speeds.append(u)

    cell = wall[0]
    slot = lax.broadcasted_iota(jnp.int32, (1, slots_all), 1)
    live = slot < count[0, 0]
    which = ref[0]
    row_hit = jnp.logical_and(
        lax.broadcasted_iota(jnp.int32, (rows, slots_all), 0) == jnp.right_shift(cell, 7), live
    )
    values = [
        jnp.right_shift(which, shift_bits) + 1,
        jnp.bitwise_and(which, slots - 1),
        jnp.right_shift(normal[0], 1),
    ]
    left = jnp.concatenate(
        [jnp.where(row_hit, value.astype(jnp.float32), 0.0) for value in values], axis=0
    ).astype(jnp.bfloat16)
    right = jnp.where(
        lax.broadcasted_iota(jnp.int32, (LANES, slots_all), 0)
        == jnp.bitwise_and(cell, LANES - 1),
        1.0,
        0.0,
    ).astype(jnp.bfloat16)
    table = lax.dot_general(
        left, right, (((1,), (1,)), ((), ())), preferred_element_type=jnp.float32
    )

    for part in range(slots_all // LANES):
        lanes = slice(part * LANES, (part + 1) * LANES)
        cells = stencil[0, 0, :, lanes]
        lane = jnp.bitwise_and(cells, LANES - 1)
        row = jnp.right_shift(cells, 7)
        picked = [jnp.zeros(cells.shape, jnp.float32)] * 3
        for r in range(rows):
            here = row == r
            for c in range(3):
                picked[c] = jnp.where(
                    here, lane_gather(vel[c * rows + r : c * rows + r + 1, :], lane), picked[c]
                )
        factor = weight[0, 0, :, lanes]
        for c in range(3):
            n = part * 3 + c
            samples[n : n + 1, :] = jnp.sum(picked[c] * factor, axis=0, keepdims=True)
    rx_row[my_y] = samples[...]

    def pairs(rho, n):
        rest = rho * equilibrium_terms(n)
        found = {13: rest}
        rho3, rho45 = (rho * 3.0, rho * 4.5)
        for i in range(13):
            s = along(n, steps[i])
            even = rest + rho45 * s * s
            odd = rho3 * s
            found[i], found[26 - i] = (even + odd, even - odd)
        return found

    coefficient = equilibrium_moments()
    rates = [jnp.broadcast_to(relax[0:1, j : j + 1], tile) for j in range(27)]
    near_rows = [
        ((a + 1) * 3 + c + 1, x)
        for a in (-1, 0, 1)
        for c in (-1, 0, 1)
        for x in range(size_x)
        if 0 <= x + a < size_x
    ]
    ends = ((0, size_x - 1), (1, 0))
    for x in range(size_x):
        found, u = (moments[x], speeds[x])
        ux, uy, uz = u
        rho, mx, my, mz = (found[0], found[9], found[3], found[1])
        owner = table[x * size_y : (x + 1) * size_y]
        place = table[rows + x * size_y : rows + (x + 1) * size_y]
        axis = table[2 * rows + x * size_y : 2 * rows + (x + 1) * size_y]
        held = jnp.where(owner > 0.5, rho, 0.0)
        code = jnp.where(owner > 0.5, (owner - 1.0) * np.float32(slots) + place + 1.0, 0.0)
        marked = solid[x].astype(jnp.float32)
        extra = [held, code, axis, marked]
        for f in range(3):
            fields[f, x] = extra[f]
        basis = [rho, mx, my, mz, mx * ux, my * uy, mz * uz, mx * uy, mx * uz, my * uz]
        deviation = []
        for j in range(27):
            if j in (0, 1, 3, 9):
                deviation.append(None)
            else:
                balance = combine(list(zip(coefficient[j], basis)))
                deviation.append(minus(found[j], balance) * rates[j])
        change = backward(deviation)
        local = pairs(held, u)
        for i in range(27):
            a, b, c = steps[i]
            half = 0.5 ** int(np.sum(steps[i] != 0)) / weights[i]
            value = pop[i, x] - change[i] * np.float32(half) - local[i]
            post[i, x] = value
            for way, edge in ends:
                if x == edge and a == 1 - 2 * way:
                    face[way, (b + 1) * 3 + c + 1] = value
            if b != 0:
                side = 0 if b > 0 else 1
                y = size_y - 1 if b > 0 else 0
                line = value[y : y + 1, :]
                j = (a + 1) * 3 + c + 1
                if (j, x) in near_rows:
                    n = near_rows.index((j, x))
                    near[side, n : n + 1, :] = line
                else:
                    corner[0 if a > 0 else 1, side, c + 1 : c + 2, :] = line
        for way, edge in ends:
            if x == edge:
                for f in range(4):
                    face[way, 9 + f] = extra[f]
        for side, y in ((0, size_y - 1), (1, 0)):
            for f in range(4):
                line = extra[f][y : y + 1, :]
                n = len(near_rows) + f * size_x + x
                near[side, n : n + 1, :] = line
                for way, edge in ends:
                    if x == edge:
                        corner[way, side, 3 + f : 4 + f, :] = line

    def send(src, dst, sem, dx, dy):
        pltpu.make_async_remote_copy(
            src_ref=src,
            dst_ref=dst,
            send_sem=send_sem,
            recv_sem=sem,
            device_id={"gx": dx, "gy": columns[dy]},
            device_id_type=MESH,
        ).start()


    used = 3 * slots_all // LANES

    def send_to(way, dy):
        dx = wrap(my_x + 1 - 2 * way, devices_x)
        send(samples.at[0:used], rx_x.at[way, my_y, 0:used], far_sem.at[way], dx, dy)
        for side, corner_dy in ((0, 1), (1, devices_y - 1)):
            if dy == corner_dy:
                send(corner.at[way, side], got_corner.at[way, side], far_sem.at[way], dx, dy)
        if dy == 0:
            sem = far_sem.at[1] if way else face_sem
            send(face.at[way], got_face.at[way], sem, dx, dy)

    def expect(sem, amount):
        pl.when(amount > 0)(lambda: pl.semaphore_wait(sem, amount))

    def both(first, second):
        return jnp.logical_and(first, second)

    def send_near():
        for side, dy in ((0, 1), (1, -1)):
            send(near.at[side], got_near.at[side], near_sem, my_x, dy)
        for dy in across:
            if dy != 0:
                send(samples.at[0:used], rx_row.at[my_y, 0:used], near_sem, my_x, dy)

    def send_where(way, chosen):
        for dy in across:
            pl.when(chosen[dy])(lambda dy=dy: send_to(way, dy))

    inside = {dy: columns[dy] < outer for dy in across}
    beyond = {dy: columns[dy] >= outer for dy in across}
    beneath = {dy: both(columns[dy] >= inner, columns[dy] < outer) for dy in across}
    top = devices_y - 2
    low = my_y < top
    ahead = [(at_last, 1, 0, 0), (my_x > 0, -1, 1, 2)]
    expect(
        barrier,
        my_y + jnp.where(my_x > 0, below, 0) + jnp.where(at_last, below, 0),
    )
    for applies, dx, way, n in ahead:

        @pl.when(applies)
        def _(dx=dx, way=way, n=n):
            if way == 0:
                send_where(way, inside)
            for dy in across:
                when(beneath[dy], ready.at[n], dx, dy)
                when(columns[dy] < inner, ready.at[n + 1], dx, dy)
            if way == 1:
                send_where(way, inside)

    for dy in range(1, devices_y):
        crossing = both(jnp.logical_not(low), columns[dy] < top) if dy % 2 == 0 else None
        lower = my_y + dy >= devices_y
        if crossing is None:
            when(lower, row_ready, 0, dy)
        else:
            when(crossing, cross, 0, dy)
            when(both(lower, jnp.logical_not(crossing)), row_ready, 0, dy)

    @pl.when(low)
    def _():
        pl.semaphore_wait(cross, 1)
        for applies, dx, way, n in ahead:

            @pl.when(applies)
            def _(way=way):
                send_where(way, beyond)

    expect(row_ready, devices_y - 1 - my_y - jnp.where(low, 1, 0))
    send_near()

    @pl.when(my_x < last)
    def _():
        pl.semaphore_wait(ready.at[2], below - inner)
        send_where(0, inside)
        expect(ready.at[3], devices_y - below)
        send_where(0, beyond)

    def spread(line):
        return jnp.broadcast_to(line, tile)

    part, offset = part_of(my_y, slots)

    near_total = 2 * near.shape[1] + (devices_y - 1) * used
    near_count = pltpu.make_async_copy(
        tally.at[0 : near_total],
        tally.at[0 : near_total],
        near_sem,
    )
    near_count.wait()
    for x in range(size_x):
        n = lookup(
            devices_y,
            *decode(fields[1, x], slots, offset),
            fields[2, x],
            lambda peer, c: spread(rx_row[peer, pl.ds(part + c, 1), :]),
        )
        found = pairs(fields[0, x], n)
        for i in range(27):
            _, b, c = steps[i]
            value = post[i, x] + found[i]
            settled[i, x] = value
            shifted[i, x] = roll(roll(value, b, 0), c, 1)

    for side in range(2):
        for n, (j, x) in enumerate(near_rows):
            q = side * size_x + x
            lines[j, q : q + 1, :] = got_near[side, n : n + 1, :]
        for f in range(4):
            for x in range(size_x):
                n = len(near_rows) + f * size_x + x
                q = side * size_x + x
                lines[9 + f, q : q + 1, :] = got_near[side, n : n + 1, :]
    lower = row_line < size_x
    part0, offset0 = part_of(columns[-1], slots)
    part1, offset1 = part_of(columns[1], slots)
    n = lookup(
        devices_y,
        *decode(lines[10], slots, jnp.where(lower, offset0, offset1)),
        lines[11],
        lambda peer, c: jnp.where(
            lower,
            spread(rx_row[peer, pl.ds(part0 + c, 1), :]),
            spread(rx_row[peer, pl.ds(part1 + c, 1), :]),
        ),
    )
    sign_b = jnp.where(lower, 1.0, -1.0)
    n[1] = n[1] * sign_b
    rho = lines[9]
    rest = equilibrium_terms(n)
    border = []
    for j in range(9):
        a, c = (j // 3 - 1, j % 3 - 1)
        s = along(n, (a, 1, c))
        border.append(roll(lines[j] + rho * (rest + s * (3.0 + 4.5 * s)), c, 1))
    marked = [roll(lines[12], c, 1) for c in (-1, 0, 1)]
    for x in range(size_x):
        plane = solid[x].astype(jnp.float32)
        for b in (-1, 0, 1):
            turned = roll(plane, b, 0)
            for c in (-1, 0, 1):
                value = roll(turned, c, 1)
                if b != 0:
                    q = (0 if b > 0 else 1) * size_x + x
                    value = mend(value, marked[c + 1][q : q + 1, :], b)
                masks[(b + 1) * 3 + c + 1, x] = value
    for i in range(27):
        a, b, c = steps[i]
        k = (b + 1) * 3 + c + 1
        for x in range(size_x):
            origin = x - a
            if 0 <= origin < size_x:
                value = shifted[i, origin]
                if b != 0:
                    q = (0 if b > 0 else 1) * size_x + origin
                    value = mend(value, border[(a + 1) * 3 + c + 1][q : q + 1, :], b)
                out[i, x] = jnp.where(masks[k, origin] != 0, settled[26 - i, x], value)

    @pl.when(my_x == 0)
    def _():
        pl.semaphore_wait(ready.at[0], below - inner)
        send_where(1, inside)
        expect(ready.at[1], devices_y - below)
        send_where(1, beyond)

    far_total = devices_y * used + 2 * corner.shape[2]
    for way, a in ((1, -1), (0, 1)):
        total = far_total
        if way == 0:
            pltpu.make_async_copy(got_face.at[way], got_face.at[way], face_sem).wait()
        else:
            total += got_face.shape[1] * size_y
            pltpu.make_async_copy(tally.at[0:total], tally.at[0:total], far_sem.at[way]).wait()
        for k in range(9):
            b, c = (k // 3 - 1, k % 3 - 1)
            moved[way, k] = roll(roll(got_face[way, k], b, 0), c, 1)
            moved[way, 9 + k] = roll(roll(got_face[way, 12], b, 0), c, 1)
        if way == 0:
            pltpu.make_async_copy(tally.at[0:total], tally.at[0:total], far_sem.at[way]).wait()
        else:
            x = size_x - 1
            tiles = far_side(
                way, devices_y, slots_all, moved, got_face, got_corner, rx_x, settled, x
            )
            for k, value in enumerate(tiles):
                out[k, x] = value
    pltpu.make_async_copy(tally, tally, send_sem).wait()


def pause(out):
    out[...] = jnp.zeros_like(out)


def local(populations, relax, solid, wall_cell, wall_normal, wall_count, sample_ref, cells, factors):
    devices_x, devices_y = (lax.axis_size("gx"), lax.axis_size("gy"))
    size_x, size_y, size_z = populations.shape[1:]
    slots_all = wall_cell.shape[2]
    slots = slots_all // devices_y
    assert size_z == LANES and LANES % slots == 0 and slots & (slots - 1) == 0
    assert slots_all % LANES == 0 and devices_x > 2 and devices_y > 2
    assert devices_y % 2 == 0
    assert 1 < size_x and 2 * size_x <= size_y == 8
    f32 = jnp.float32
    near_lines = -(-(9 * size_x - 6 + 4 * size_x) // 8) * 8
    held = -(-3 * slots_all // LANES // 8) * 8
    used = 3 * slots_all // LANES
    sent = (3 * devices_y - 1) * used + 2 * 13 * size_y + 2 * near_lines + 4 * 8
    vmem = pltpu.VMEM
    tile = (size_y, LANES)
    on_core = pl.BlockSpec(memory_space=pltpu.VMEM)
    scalars = pl.BlockSpec(memory_space=pltpu.SMEM)

    def near_core(value):
        return pltpu.with_memory_space_constraint(value, pltpu.VMEM)

    dma = pltpu.SemaphoreType.DMA
    regular = pltpu.SemaphoreType.REGULAR
    gate = pl.pallas_call(
        pause,
        out_shape=pltpu.VMEM(tile, f32),
        out_specs=pl.BlockSpec(memory_space=pltpu.VMEM),
        cost_estimate=pl.CostEstimate(flops=10**9, bytes_accessed=4096, transcendentals=0),
        name="pause",
    )()
    kept = [
        populations.shape,
        populations.shape,
        (2, 18) + tile,
        (2, 13) + tile,
        (2, 2, 8, LANES),
        (2, devices_y, held, LANES),
    ]
    results = pl.pallas_call(
        functools.partial(kernel, devices_x, devices_y),
        out_shape=[pltpu.VMEM(shape, f32) for shape in kept],
        in_specs=[on_core] * 6 + [scalars] + [on_core] * 3,
        out_specs=[on_core] * len(kept),
        scratch_shapes=[
            vmem((3 * size_x * size_y, LANES), f32),
            vmem((held, LANES), f32),
            vmem((devices_y, held, LANES), f32),
            vmem(populations.shape, f32),
            vmem(populations.shape, f32),
            vmem((3, size_x) + tile, f32),
            vmem((2, 13) + tile, f32),
            vmem((2, near_lines, LANES), f32),
            vmem((2, 2, 8, LANES), f32),
            vmem((2, near_lines, LANES), f32),
            vmem((13,) + tile, f32),
            vmem((9, size_x) + tile, f32),
            vmem((sent, LANES), f32),
            dma,
            dma,
            dma,
            dma((2,)),
            regular,
            regular,
            regular((4,)),
        ],
        compiler_params=pltpu.CompilerParams(collective_id=0, has_side_effects=True),
        name="lattice_step",
    )(
        pltpu.with_memory_space_constraint(gate, pltpu.VMEM),
        near_core(populations),
        near_core(relax.reshape(1, 27)),
        near_core(solid),
        near_core(wall_cell),
        near_core(wall_normal),
        wall_count,
        near_core(sample_ref),
        near_core(cells),
        near_core(factors),
    )
    return pl.pallas_call(
        functools.partial(finish, devices_y, slots_all),
        out_shape=jax.ShapeDtypeStruct(populations.shape, f32),
        in_specs=[on_core] * len(kept),
        out_specs=pl.BlockSpec(memory_space=pl.ANY),
        scratch_shapes=[vmem((9,) + tile, f32), dma((3,))],
        name="finish",
    )(*[near_core(value) for value in results])


def solution(mesh):
    return jax.shard_map(
        local,
        mesh=mesh,
        in_specs=(
            P(None, "gx", "gy", None),
            P(),
            P("gx", "gy", None),
            P("gx", "gy", None),
            P("gx", "gy", None),
            P("gx", "gy"),
            P("gx", "gy", None),
            P("gx", "gy", None, None),
            P("gx", "gy", None, None),
        ),
        out_specs=P(None, "gx", "gy", None),
        check_vma=False,
    )
```

```python
import functools

import jax
import jax.numpy as jnp
import numpy as np
from jax import lax
from jax.experimental import pallas as pl
from jax.experimental.pallas import tpu as pltpu
from jax.sharding import PartitionSpec as P


steps = np.array([(a - 1, b - 1, c - 1) for a in range(3) for b in range(3) for c in range(3)])
wall_ratio = (1.0 / 9.0) ** (1.0 / 7.0)
weights = np.prod(np.where(steps == 0, 2.0 / 3.0, 1.0 / 6.0), axis=1)
vander = np.array([[1.0, 1.0, 1.0], [-1.0, 0.0, 1.0], [1.0, 0.0, 1.0]])
moment = np.kron(np.kron(vander, vander), vander)
LANES = 128
MESH = pl.DeviceIdType.MESH


def equilibrium_moments():
    x, y, z = steps.T.astype(float)
    basis = np.stack(
        [
            np.ones(27),
            3 * x,
            3 * y,
            3 * z,
            4.5 * x * x - 1.5,
            4.5 * y * y - 1.5,
            4.5 * z * z - 1.5,
            9 * x * y,
            9 * x * z,
            9 * y * z,
        ],
        axis=1,
    )
    return moment @ (weights[:, None] * basis)


def forward(vals):
    for stride in (9, 3, 1):
        out = list(vals)
        for i in range(27):
            if i // stride % 3 == 0:
                lo, mid, hi = (vals[i], vals[i + stride], vals[i + 2 * stride])
                both = lo + hi
                out[i], out[i + stride], out[i + 2 * stride] = (both + mid, hi - lo, both)
        vals = out
    return vals


def plus(a, b):
    return b if a is None else a if b is None else a + b


def minus(a, b):
    return a if b is None else -b if a is None else a - b


def backward(vals):
    for stride in (9, 3, 1):
        out = list(vals)
        for i in range(27):
            if i // stride % 3 == 0:
                s0, s1, s2 = (vals[i], vals[i + stride], vals[i + 2 * stride])
                out[i], out[i + stride], out[i + 2 * stride] = (
                    minus(s2, s1),
                    minus(s0, s2),
                    plus(s2, s1),
                )
        vals = out
    return vals


def combine(terms):
    total = None
    for factor, value in terms:
        if abs(factor) < 1e-12:
            continue
        if abs(factor - 1.0) < 1e-12:
            total = plus(total, value)
        elif abs(factor + 1.0) < 1e-12:
            total = minus(total, value)
        else:
            total = plus(total, value * np.float32(factor))
    return total


def roll(value, shift, axis):
    return value if shift == 0 else pltpu.roll(value, shift % value.shape[axis], axis)


def lane_gather(row, index):
    return jnp.take_along_axis(
        jnp.broadcast_to(row, index.shape), index, axis=1, mode="promise_in_bounds"
    )


def equilibrium_terms(n):
    square = [value * value for value in n]
    return 1.0 - 1.5 * (square[0] + square[1] + square[2])


def along(n, step):
    total = None
    for c in range(3):
        if step[c] > 0:
            total = plus(total, n[c])
        elif step[c] < 0:
            total = minus(total, n[c])
    return total


def decode(code, slots, offset):
    r = code.astype(jnp.int32) - 1
    owner = jnp.right_shift(r, slots.bit_length() - 1)
    return owner, jnp.bitwise_and(r, slots - 1) + offset


def lookup(devices_y, owner, lane, axis, operand):
    value = [jnp.zeros(lane.shape, jnp.float32)] * 3
    for peer in range(devices_y):
        here = owner == peer
        for c in range(3):
            value[c] = jnp.where(
                here,
                jnp.take_along_axis(operand(peer, c), lane, axis=1, mode="promise_in_bounds"),
                value[c],
            )
    ratio = np.float32(wall_ratio)
    return [jnp.where(axis == np.float32(c), 0.0, value[c] * ratio) for c in range(3)]


def wrap(value, size):
    return jnp.where(value < 0, value + size, jnp.where(value >= size, value - size, value))


def part_of(owner, slots):
    return (owner * slots) // LANES * 3, lax.rem(owner * slots, LANES)


def mend(value, line, b):
    size_y = value.shape[0]
    row_line = lax.broadcasted_iota(jnp.int32, value.shape, 0)
    edge = 0 if b > 0 else size_y - 1
    return jnp.where(row_line == edge, jnp.broadcast_to(line, value.shape), value)


def far_side(way, devices_y, slots_all, moved, got_face, got_corner, rx_x, settled, x):
    a = 1 - 2 * way
    tile = got_face.shape[2:]
    slots = slots_all // devices_y
    my_y = lax.axis_index("gy")
    part, offset = part_of(my_y, slots)
    part0, offset0 = part_of(wrap(my_y - 1, devices_y), slots)
    part1, offset1 = part_of(wrap(my_y + 1, devices_y), slots)
    upper = lax.broadcasted_iota(jnp.int32, tile, 0) == 0

    def spread(line):
        return jnp.broadcast_to(line, tile)

    def stack(one, other):
        return jnp.where(upper, spread(one), spread(other))

    quantity = [
        stack(got_corner[way, 0, f : f + 1, :], got_corner[way, 1, f : f + 1, :]) for f in range(7)
    ]
    n = lookup(
        devices_y,
        *decode(quantity[4], slots, jnp.where(upper, offset0, offset1)),
        quantity[5],
        lambda peer, c: stack(
            rx_x[way, peer, pl.ds(part0 + c, 1), :], rx_x[way, peer, pl.ds(part1 + c, 1), :]
        ),
    )
    n[1] = jnp.where(upper, n[1], -n[1])
    rest = equilibrium_terms(n)
    corners, marked = ([], [])
    for c in (-1, 0, 1):
        s = along(n, (a, 1, c))
        value = quantity[c + 1] + quantity[3] * (rest + s * (3.0 + 4.5 * s))
        corners.append(roll(value, c, 1))
        marked.append(roll(quantity[6], c, 1))
    n = lookup(
        devices_y,
        *decode(got_face[way, 10], slots, offset),
        got_face[way, 11],
        lambda peer, c: spread(rx_x[way, peer, pl.ds(part + c, 1), :]),
    )
    rho = got_face[way, 9]
    rest = equilibrium_terms(n)
    tiles = []
    for k in range(9):
        b, c = (k // 3 - 1, k % 3 - 1)
        i = (a + 1) * 9 + k
        s = along(n, (a, b, c))
        value = moved[way, k] + roll(roll(rho * (rest + s * (3.0 + 4.5 * s)), b, 0), c, 1)
        mark = moved[way, 9 + k]
        if b != 0:
            q = 0 if b > 0 else 1
            value = mend(value, corners[c + 1][q : q + 1, :], b)
            mark = mend(mark, marked[c + 1][q : q + 1, :], b)
        tiles.append(jnp.where(mark != 0, settled[26 - i, x], value))
    return tiles


def finish(devices_y, slots_all, early, settled, moved, got_face, got_corner, rx_x, out, late, sem):
    copies = [
        pltpu.make_async_copy(early.at[0:18], out.at[0:18], sem.at[0]),
        pltpu.make_async_copy(early.at[18:27, 1:], out.at[18:27, 1:], sem.at[1]),
        pltpu.make_async_copy(late, out.at[18:27, 0], sem.at[2]),
    ]
    copies[0].start()
    copies[1].start()
    tiles = far_side(0, devices_y, slots_all, moved, got_face, got_corner, rx_x, settled, 0)
    for k, value in enumerate(tiles):
        late[k] = value
    copies[2].start()
    for copy in copies:
        copy.wait()


def kernel(
    devices_x,
    devices_y,
    gate,
    pop,
    relax,
    solid,
    wall,
    normal,
    count,
    ref,
    stencil,
    weight,
    out,
    settled,
    moved,
    got_face,
    got_corner,
    rx_x,
    vel,
    samples,
    rx_row,
    post,
    shifted,
    fields,
    face,
    near,
    corner,
    got_near,
    lines,
    masks,
    tally,
    send_sem,
    near_sem,
    face_sem,
    far_sem,
    row_ready,
    ready,
):
    size_x, size_y = pop.shape[1:3]
    rows = size_x * size_y
    slots_all = wall.shape[2]
    slots = slots_all // devices_y
    shift_bits = slots.bit_length() - 1
    my_x = lax.axis_index("gx")
    my_y = lax.axis_index("gy")
    tile = (size_y, LANES)

    barrier = pltpu.get_barrier_semaphore()
    columns = {dy: wrap(my_y + dy, devices_y) for dy in range(devices_y)}
    columns[-1] = columns[devices_y - 1]
    beside = {dx: wrap(my_x + dx, devices_x) for dx in (-1, 0, 1)}
    last = devices_x - 1
    inner = my_y - jnp.bitwise_and(my_y, 1)
    outer = inner + 2
    below = jnp.minimum(outer, devices_y)

    def tell(sem, dx, dy):
        pl.semaphore_signal(
            sem,
            inc=1,
            device_id={"gx": beside[dx], "gy": columns[dy]},
            device_id_type=MESH,
        )

    def when(condition, *signal):
        pl.when(condition)(lambda: tell(*signal))

    at_last = my_x == last
    inward = jnp.where(my_x == 0, inner, devices_y)
    outward = jnp.where(at_last, devices_y, inner)
    across = sorted(range(devices_y), key=lambda dy: -min(dy, devices_y - dy))
    for dy in across:

        @pl.when(columns[dy] >= inward)
        def _(dy=dy):
            pl.semaphore_signal(
                barrier,
                inc=1,
                device_id={"gx": last, "gy": columns[dy]},
                device_id_type=MESH,
            )

    for dy in across:
        when(columns[dy] >= outward, barrier, 1, dy)
    for dy in range(1, devices_y):
        when(my_y + dy < devices_y, barrier, 0, dy)

    row_line = lax.broadcasted_iota(jnp.int32, tile, 0)

    moments, speeds = ([], [])
    for x in range(size_x):
        found = forward([pop[i, x] * np.float32(weights[i]) for i in range(27)])
        rho = found[0]
        inverse = 1.0 / rho
        u = [found[9] * inverse, found[3] * inverse, found[1] * inverse]
        for c in range(3):
            vel[c * rows + x * size_y : c * rows + (x + 1) * size_y, :] = u[c]
        moments.append(found)
        speeds.append(u)

    cell = wall[0]
    slot = lax.broadcasted_iota(jnp.int32, (1, slots_all), 1)
    live = slot < count[0, 0]
    which = ref[0]
    row_hit = jnp.logical_and(
        lax.broadcasted_iota(jnp.int32, (rows, slots_all), 0) == jnp.right_shift(cell, 7), live
    )
    values = [
        jnp.right_shift(which, shift_bits) + 1,
        jnp.bitwise_and(which, slots - 1),
        jnp.right_shift(normal[0], 1),
    ]
    left = jnp.concatenate(
        [jnp.where(row_hit, value.astype(jnp.float32), 0.0) for value in values], axis=0
    ).astype(jnp.bfloat16)
    right = jnp.where(
        lax.broadcasted_iota(jnp.int32, (LANES, slots_all), 0)
        == jnp.bitwise_and(cell, LANES - 1),
        1.0,
        0.0,
    ).astype(jnp.bfloat16)
    table = lax.dot_general(
        left, right, (((1,), (1,)), ((), ())), preferred_element_type=jnp.float32
    )

    for part in range(slots_all // LANES):
        lanes = slice(part * LANES, (part + 1) * LANES)
        cells = stencil[0, 0, :, lanes]
        lane = jnp.bitwise_and(cells, LANES - 1)
        row = jnp.right_shift(cells, 7)
        picked = [jnp.zeros(cells.shape, jnp.float32)] * 3
        for r in range(rows):
            here = row == r
            for c in range(3):
                picked[c] = jnp.where(
                    here, lane_gather(vel[c * rows + r : c * rows + r + 1, :], lane), picked[c]
                )
        factor = weight[0, 0, :, lanes]
        for c in range(3):
            n = part * 3 + c
            samples[n : n + 1, :] = jnp.sum(picked[c] * factor, axis=0, keepdims=True)
    rx_row[my_y] = samples[...]

    def pairs(rho, n):
        rest = rho * equilibrium_terms(n)
        found = {13: rest}
        rho3, rho45 = (rho * 3.0, rho * 4.5)
        for i in range(13):
            s = along(n, steps[i])
            even = rest + rho45 * s * s
            odd = rho3 * s
            found[i], found[26 - i] = (even + odd, even - odd)
        return found

    coefficient = equilibrium_moments()
    rates = [jnp.broadcast_to(relax[0:1, j : j + 1], tile) for j in range(27)]
    near_rows = [
        ((a + 1) * 3 + c + 1, x)
        for a in (-1, 0, 1)
        for c in (-1, 0, 1)
        for x in range(size_x)
        if 0 <= x + a < size_x
    ]
    ends = ((0, size_x - 1), (1, 0))
    for x in range(size_x):
        found, u = (moments[x], speeds[x])
        ux, uy, uz = u
        rho, mx, my, mz = (found[0], found[9], found[3], found[1])
        owner = table[x * size_y : (x + 1) * size_y]
        place = table[rows + x * size_y : rows + (x + 1) * size_y]
        axis = table[2 * rows + x * size_y : 2 * rows + (x + 1) * size_y]
        held = jnp.where(owner > 0.5, rho, 0.0)
        code = jnp.where(owner > 0.5, (owner - 1.0) * np.float32(slots) + place + 1.0, 0.0)
        marked = solid[x].astype(jnp.float32)
        extra = [held, code, axis, marked]
        for f in range(3):
            fields[f, x] = extra[f]
        basis = [rho, mx, my, mz, mx * ux, my * uy, mz * uz, mx * uy, mx * uz, my * uz]
        deviation = []
        for j in range(27):
            if j in (0, 1, 3, 9):
                deviation.append(None)
            else:
                balance = combine(list(zip(coefficient[j], basis)))
                deviation.append(minus(found[j], balance) * rates[j])
        change = backward(deviation)
        local = pairs(held, u)
        for i in range(27):
            a, b, c = steps[i]
            half = 0.5 ** int(np.sum(steps[i] != 0)) / weights[i]
            value = pop[i, x] - change[i] * np.float32(half) - local[i]
            post[i, x] = value
            for way, edge in ends:
                if x == edge and a == 1 - 2 * way:
                    face[way, (b + 1) * 3 + c + 1] = value
            if b != 0:
                side = 0 if b > 0 else 1
                y = size_y - 1 if b > 0 else 0
                line = value[y : y + 1, :]
                j = (a + 1) * 3 + c + 1
                if (j, x) in near_rows:
                    n = near_rows.index((j, x))
                    near[side, n : n + 1, :] = line
                else:
                    corner[0 if a > 0 else 1, side, c + 1 : c + 2, :] = line
        for way, edge in ends:
            if x == edge:
                for f in range(4):
                    face[way, 9 + f] = extra[f]
        for side, y in ((0, size_y - 1), (1, 0)):
            for f in range(4):
                line = extra[f][y : y + 1, :]
                n = len(near_rows) + f * size_x + x
                near[side, n : n + 1, :] = line
                for way, edge in ends:
                    if x == edge:
                        corner[way, side, 3 + f : 4 + f, :] = line

    def send(src, dst, sem, dx, dy):
        pltpu.make_async_remote_copy(
            src_ref=src,
            dst_ref=dst,
            send_sem=send_sem,
            recv_sem=sem,
            device_id={"gx": dx, "gy": columns[dy]},
            device_id_type=MESH,
        ).start()


    used = 3 * slots_all // LANES

    def send_to(way, dy):
        dx = wrap(my_x + 1 - 2 * way, devices_x)
        send(samples.at[0:used], rx_x.at[way, my_y, 0:used], far_sem.at[way], dx, dy)
        for side, corner_dy in ((0, 1), (1, devices_y - 1)):
            if dy == corner_dy:
                send(corner.at[way, side], got_corner.at[way, side], far_sem.at[way], dx, dy)
        if dy == 0:
            sem = far_sem.at[1] if way else face_sem
            send(face.at[way], got_face.at[way], sem, dx, dy)

    def expect(sem, amount):
        pl.when(amount > 0)(lambda: pl.semaphore_wait(sem, amount))

    def both(first, second):
        return jnp.logical_and(first, second)

    def send_near():
        for side, dy in ((0, 1), (1, -1)):
            send(near.at[side], got_near.at[side], near_sem, my_x, dy)
        for dy in across:
            if dy != 0:
                send(samples.at[0:used], rx_row.at[my_y, 0:used], near_sem, my_x, dy)

    def send_where(way, chosen):
        for dy in across:
            pl.when(chosen[dy])(lambda dy=dy: send_to(way, dy))

    inside = {dy: columns[dy] < outer for dy in across}
    beyond = {dy: columns[dy] >= outer for dy in across}
    beneath = {dy: both(columns[dy] >= inner, columns[dy] < outer) for dy in across}
    top = devices_y - 2
    low = both(my_y < top, my_x > 0)
    high = both(my_y >= top, my_x > 0)
    ahead = [(at_last, 1, 0, 0), (my_x > 0, -1, 1, 2)]
    expect(
        barrier,
        my_y + jnp.where(my_x > 0, below, 0) + jnp.where(at_last, below, 0),
    )
    for applies, dx, way, n in ahead:

        @pl.when(applies)
        def _(dx=dx, way=way, n=n):
            if way == 0:
                send_where(way, inside)
            for dy in across:
                when(beneath[dy], ready.at[n], dx, dy)
                when(columns[dy] < inner, ready.at[n + 1], dx, dy)
            if way == 1:
                send_where(way, inside)

    for dy in range(1, devices_y):
        crossing = both(high, columns[dy] < top) if dy % 2 == 0 else None
        lower = my_y + dy >= devices_y
        if crossing is None:
            when(lower, row_ready, 0, dy)
        else:
            when(crossing, ready.at[0], 0, dy)
            when(both(lower, jnp.logical_not(crossing)), row_ready, 0, dy)

    @pl.when(low)
    def _():
        pl.semaphore_wait(ready.at[0], 1)
        for applies, dx, way, n in ahead:

            @pl.when(applies)
            def _(way=way):
                send_where(way, beyond)

    expect(row_ready, devices_y - 1 - my_y - jnp.where(low, 1, 0))
    send_near()

    @pl.when(my_x < last)
    def _():
        pl.semaphore_wait(ready.at[2], below - inner)
        send_where(0, inside)
        expect(ready.at[3], devices_y - below)
        send_where(0, beyond)

    def spread(line):
        return jnp.broadcast_to(line, tile)

    part, offset = part_of(my_y, slots)

    near_total = 2 * near.shape[1] + (devices_y - 1) * used
    near_count = pltpu.make_async_copy(
        tally.at[0 : near_total],
        tally.at[0 : near_total],
        near_sem,
    )
    near_count.wait()
    for x in range(size_x):
        n = lookup(
            devices_y,
            *decode(fields[1, x], slots, offset),
            fields[2, x],
            lambda peer, c: spread(rx_row[peer, pl.ds(part + c, 1), :]),
        )
        found = pairs(fields[0, x], n)
        for i in range(27):
            _, b, c = steps[i]
            value = post[i, x] + found[i]
            settled[i, x] = value
            shifted[i, x] = roll(roll(value, b, 0), c, 1)

    for side in range(2):
        for n, (j, x) in enumerate(near_rows):
            q = side * size_x + x
            lines[j, q : q + 1, :] = got_near[side, n : n + 1, :]
        for f in range(4):
            for x in range(size_x):
                n = len(near_rows) + f * size_x + x
                q = side * size_x + x
                lines[9 + f, q : q + 1, :] = got_near[side, n : n + 1, :]
    lower = row_line < size_x
    part0, offset0 = part_of(columns[-1], slots)
    part1, offset1 = part_of(columns[1], slots)
    n = lookup(
        devices_y,
        *decode(lines[10], slots, jnp.where(lower, offset0, offset1)),
        lines[11],
        lambda peer, c: jnp.where(
            lower,
            spread(rx_row[peer, pl.ds(part0 + c, 1), :]),
            spread(rx_row[peer, pl.ds(part1 + c, 1), :]),
        ),
    )
    sign_b = jnp.where(lower, 1.0, -1.0)
    n[1] = n[1] * sign_b
    rho = lines[9]
    rest = equilibrium_terms(n)
    border = []
    for j in range(9):
        a, c = (j // 3 - 1, j % 3 - 1)
        s = along(n, (a, 1, c))
        border.append(roll(lines[j] + rho * (rest + s * (3.0 + 4.5 * s)), c, 1))
    marked = [roll(lines[12], c, 1) for c in (-1, 0, 1)]
    for x in range(size_x):
        plane = solid[x].astype(jnp.float32)
        for b in (-1, 0, 1):
            turned = roll(plane, b, 0)
            for c in (-1, 0, 1):
                value = roll(turned, c, 1)
                if b != 0:
                    q = (0 if b > 0 else 1) * size_x + x
                    value = mend(value, marked[c + 1][q : q + 1, :], b)
                masks[(b + 1) * 3 + c + 1, x] = value
    for i in range(27):
        a, b, c = steps[i]
        k = (b + 1) * 3 + c + 1
        for x in range(size_x):
            origin = x - a
            if 0 <= origin < size_x:
                value = shifted[i, origin]
                if b != 0:
                    q = (0 if b > 0 else 1) * size_x + origin
                    value = mend(value, border[(a + 1) * 3 + c + 1][q : q + 1, :], b)
                out[i, x] = jnp.where(masks[k, origin] != 0, settled[26 - i, x], value)

    @pl.when(my_x == 0)
    def _():
        pl.semaphore_wait(ready.at[0], below - inner)
        send_where(1, inside)
        expect(ready.at[1], devices_y - below)
        send_where(1, beyond)

    far_total = devices_y * used + 2 * corner.shape[2]
    for way, a in ((1, -1), (0, 1)):
        total = far_total
        if way == 0:
            pltpu.make_async_copy(got_face.at[way], got_face.at[way], face_sem).wait()
        else:
            total += got_face.shape[1] * size_y
            pltpu.make_async_copy(tally.at[0:total], tally.at[0:total], far_sem.at[way]).wait()
        for k in range(9):
            b, c = (k // 3 - 1, k % 3 - 1)
            moved[way, k] = roll(roll(got_face[way, k], b, 0), c, 1)
            moved[way, 9 + k] = roll(roll(got_face[way, 12], b, 0), c, 1)
        if way == 0:
            pltpu.make_async_copy(tally.at[0:total], tally.at[0:total], far_sem.at[way]).wait()
        else:
            x = size_x - 1
            tiles = far_side(
                way, devices_y, slots_all, moved, got_face, got_corner, rx_x, settled, x
            )
            for k, value in enumerate(tiles):
                out[k, x] = value
    pltpu.make_async_copy(tally, tally, send_sem).wait()


def pause(out):
    out[...] = jnp.zeros_like(out)


def local(populations, relax, solid, wall_cell, wall_normal, wall_count, sample_ref, cells, factors):
    devices_x, devices_y = (lax.axis_size("gx"), lax.axis_size("gy"))
    size_x, size_y, size_z = populations.shape[1:]
    slots_all = wall_cell.shape[2]
    slots = slots_all // devices_y
    assert size_z == LANES and LANES % slots == 0 and slots & (slots - 1) == 0
    assert slots_all % LANES == 0 and devices_x > 2 and devices_y > 2
    assert devices_y % 2 == 0
    assert 1 < size_x and 2 * size_x <= size_y == 8
    f32 = jnp.float32
    near_lines = -(-(9 * size_x - 6 + 4 * size_x) // 8) * 8
    held = -(-3 * slots_all // LANES // 8) * 8
    used = 3 * slots_all // LANES
    sent = (3 * devices_y - 1) * used + 2 * 13 * size_y + 2 * near_lines + 4 * 8
    vmem = pltpu.VMEM
    tile = (size_y, LANES)
    on_core = pl.BlockSpec(memory_space=pltpu.VMEM)
    scalars = pl.BlockSpec(memory_space=pltpu.SMEM)

    def near_core(value):
        return pltpu.with_memory_space_constraint(value, pltpu.VMEM)

    dma = pltpu.SemaphoreType.DMA
    regular = pltpu.SemaphoreType.REGULAR
    gate = pl.pallas_call(
        pause,
        out_shape=pltpu.VMEM(tile, f32),
        out_specs=pl.BlockSpec(memory_space=pltpu.VMEM),
        cost_estimate=pl.CostEstimate(flops=10**9, bytes_accessed=4096, transcendentals=0),
        name="pause",
    )()
    kept = [
        populations.shape,
        populations.shape,
        (2, 18) + tile,
        (2, 13) + tile,
        (2, 2, 8, LANES),
        (2, devices_y, held, LANES),
    ]
    results = pl.pallas_call(
        functools.partial(kernel, devices_x, devices_y),
        out_shape=[pltpu.VMEM(shape, f32) for shape in kept],
        in_specs=[on_core] * 6 + [scalars] + [on_core] * 3,
        out_specs=[on_core] * len(kept),
        scratch_shapes=[
            vmem((3 * size_x * size_y, LANES), f32),
            vmem((held, LANES), f32),
            vmem((devices_y, held, LANES), f32),
            vmem(populations.shape, f32),
            vmem(populations.shape, f32),
            vmem((3, size_x) + tile, f32),
            vmem((2, 13) + tile, f32),
            vmem((2, near_lines, LANES), f32),
            vmem((2, 2, 8, LANES), f32),
            vmem((2, near_lines, LANES), f32),
            vmem((13,) + tile, f32),
            vmem((9, size_x) + tile, f32),
            vmem((sent, LANES), f32),
            dma,
            dma,
            dma,
            dma((2,)),
            regular,
            regular((4,)),
        ],
        compiler_params=pltpu.CompilerParams(collective_id=0, has_side_effects=True),
        name="lattice_step",
    )(
        pltpu.with_memory_space_constraint(gate, pltpu.VMEM),
        near_core(populations),
        near_core(relax.reshape(1, 27)),
        near_core(solid),
        near_core(wall_cell),
        near_core(wall_normal),
        wall_count,
        near_core(sample_ref),
        near_core(cells),
        near_core(factors),
    )
    return pl.pallas_call(
        functools.partial(finish, devices_y, slots_all),
        out_shape=jax.ShapeDtypeStruct(populations.shape, f32),
        in_specs=[on_core] * len(kept),
        out_specs=pl.BlockSpec(memory_space=pl.ANY),
        scratch_shapes=[vmem((9,) + tile, f32), dma((3,))],
        name="finish",
    )(*[near_core(value) for value in results])


def solution(mesh):
    return jax.shard_map(
        local,
        mesh=mesh,
        in_specs=(
            P(None, "gx", "gy", None),
            P(),
            P("gx", "gy", None),
            P("gx", "gy", None),
            P("gx", "gy", None),
            P("gx", "gy"),
            P("gx", "gy", None),
            P("gx", "gy", None, None),
            P("gx", "gy", None, None),
        ),
        out_specs=P(None, "gx", "gy", None),
        check_vma=False,
    )
```
